32 devices in a mesh: gx: 4 (over y, x), gy: 4 (over z), gz: 2 (over core).
Axes of the slice: x: 2, y: 2, z: 4, core: 2. Of those that a mesh axis runs over, the one named last changes fastest.
Arguments:
- hidden: bfloat16 [4096, 2, 4096], P(('gx', 'gy', 'gz')), may hold values from -6 to 6
- norm_gain: float32 [4096], replicated, may hold values from 0.25 to 1.75
- prompt_of: int32 [4096], P(('gx', 'gy', 'gz')), may hold values from 0 to 255, as said below
- lengths: int32 [4096], P(('gx', 'gy', 'gz')), may hold values from 1 to 2
- reward_level: int32 [4096], P(('gx', 'gy', 'gz')), may hold values from 0 to 15
Outputs:
- weighted: bfloat16 [4096, 2, 4096], P(('gx', 'gy', 'gz'))
- advantages: float32 [4096], P(('gx', 'gy', 'gz'))
The draws below stay inside these ranges and needn't reach their ends.
Inputs may be any that keep to these rules, and one draw needn't show every extreme that they name: `prompt_of`: each of the 256 prompts has exactly 16 completions; prompt p is owned by the device p // 8 in mesh order; the completions of one device include at most 5 whose prompts one owner holds, and exactly 5 for some owner.
All inputs are finite; a program needn't handle non-finite values.
Results may differ from the reference program's by a relative error of at most 0.0085.
Values may be sent and summed in bfloat16 or wider, within the bound.
No kernel may reach another device: no remote copies, remote signals or barrier semaphores. Data moves between devices by JAX's collectives and lax.ppermute only.
A program may use at most 64 MiB of HBM per device.

```python
import jax
import jax.numpy as jnp
from jax import lax

D = 4096
G = 16
P_DEV = 8
W = 2
OWNERS = 32
COMP_DEV = 128
SLOTS = 5
COMPLETIONS = 4096
PROMPTS = 256


def regroup_plan(key):
    plan_key = jax.random.fold_in(key, 7301)
    key_offsets, key_shift, key_member, key_tiebreak = jax.random.split(plan_key, 4)
    chosen = jax.random.permutation(key_offsets, OWNERS)
    member_index = jnp.arange(COMP_DEV, dtype=jnp.int32)
    spread_index = jnp.where(member_index < SLOTS, 0, 1 + (member_index - SLOTS) % (OWNERS - 1))
    offsets = chosen[spread_index]
    owner_shift = jax.random.permutation(key_shift, OWNERS)

    def member_order(member_key):
        return jax.random.permutation(member_key, COMP_DEV)
    member_perm = jax.vmap(member_order)(jax.random.split(key_member, OWNERS))
    target_device = (owner_shift[:, None] + offsets[member_perm]) % OWNERS
    prompt_ids = jnp.arange(OWNERS, dtype=jnp.int32)[:, None] * P_DEV + jnp.arange(COMP_DEV, dtype=jnp.int32)[None, :] // G
    tiebreak = jax.random.permutation(key_tiebreak, COMPLETIONS)
    scores = target_device.reshape(-1) * COMPLETIONS + tiebreak
    arranged = jnp.argsort(scores)
    return prompt_ids.reshape(-1)[arranged].astype(jnp.int32)


def draw_prompt_of(key, part):
    return regroup_plan(key)


def draw_reward_level(key, part):
    prompt_ids = regroup_plan(key)
    key_base, key_spread, key_jitter = jax.random.split(jax.random.fold_in(key, 911), 3)
    base_level = jax.random.randint(key_base, (PROMPTS,), 0, 9)
    spread = jax.random.randint(key_spread, (PROMPTS,), 1, 9)
    jitter = jax.random.randint(key_jitter, (COMPLETIONS,), 0, 65536) % spread[prompt_ids]
    return (base_level[prompt_ids] + jitter).astype(jnp.int32)


def set_ends(values, key, smallest, high):
    spot = [jax.random.randint(jax.random.fold_in(key, axis), (), 0, length) for axis, length in enumerate(values.shape)]
    widest = values.shape.index(max(values.shape))
    neighbour = spot[:widest] + [(spot[widest] + 1) % values.shape[widest]] + spot[widest + 1:]
    return values.at[tuple(spot)].set(smallest).at[tuple(neighbour)].set(high)


def block_scale(key, dims, cuts, smallest, high):
    factor_of, own = 1.0, jax.random.fold_in(key, 6)
    for position, blocks in cuts:
        heights = jnp.exp(jax.random.uniform(jax.random.fold_in(own, position), (blocks,), jnp.float32, smallest / len(cuts), high / len(cuts)))
        factor_of = factor_of * jnp.repeat(heights, dims[position] // blocks).reshape([-1 if axis == position else 1 for axis in range(len(dims))])
    return factor_of


def centred(key, shape, scale, reach, pieces=(), kind=jnp.bfloat16):
    gain = block_scale(key, shape, pieces, -0.22, 0.18) if pieces else 1.0
    result = jax.random.normal(key, shape, jnp.float32) * scale * gain
    return jnp.minimum(jnp.maximum(result, -reach), reach).astype(kind)


def setup_inputs(seed: int = 0) -> dict:
    seeds = jax.random.split(jax.random.key(seed), 6)
    hidden = centred(seeds[0], (COMPLETIONS, W, D), 1.0, 6.0, ((0, 32),))
    norm_gain = jnp.clip(1.0 + 0.15 * jax.random.normal(seeds[1], (D,), jnp.float32), 0.25, 1.75)
    prompt_of = draw_prompt_of(jax.random.fold_in(seeds[5], 71), 0)
    lengths = set_ends(jax.random.randint(seeds[3], (COMPLETIONS,), 1, W + 1), jax.random.fold_in(seeds[3], 1), 1, W).astype(jnp.int32)
    reward_level = draw_reward_level(jax.random.fold_in(seeds[5], 71), 0)
    return dict(hidden=hidden, norm_gain=norm_gain, prompt_of=prompt_of, lengths=lengths, reward_level=reward_level)


norm_eps = 1e-05

def normalize(block, norm_gain):
    values = block.astype(jnp.float32)
    meansq = lax.optimization_barrier(jnp.mean(values * values, axis=-1, keepdims=True))
    return (values * lax.rsqrt(meansq + norm_eps) * norm_gain.astype(jnp.float32)).astype(jnp.bfloat16)

def reference(hidden, norm_gain, prompt_of, lengths, reward_level):
    blocks = hidden.reshape(OWNERS, COMP_DEV, W, D)

    def norm_block(block):
        return normalize(block, norm_gain)
    normed = lax.map(norm_block, blocks).reshape(COMPLETIONS, W, D)
    ordering = jnp.argsort(prompt_of, stable=True).astype(jnp.int32)
    normed = normed[ordering]
    levels = reward_level[ordering].astype(jnp.float32).reshape(PROMPTS, G)
    average = lax.optimization_barrier(jnp.mean(levels, axis=1, keepdims=True))
    centered = levels - average
    spread = jnp.sqrt(lax.optimization_barrier(jnp.mean(centered * centered, axis=1, keepdims=True)))
    advantages = (centered / jnp.maximum(spread, 1.0)).reshape(COMPLETIONS)
    lengths_sorted = lengths[ordering]
    tokens_at = jnp.arange(W, dtype=jnp.int32)
    weight = jnp.where(tokens_at[None, :] < lengths_sorted[:, None], advantages[:, None] / lengths_sorted[:, None].astype(jnp.float32), 0.0)

    def scale_block(pair):
        block, block_weight = pair
        return (block.astype(jnp.float32) * block_weight[:, :, None]).astype(jnp.bfloat16)
    weighted = lax.map(scale_block, (normed.reshape(OWNERS, COMP_DEV, W, D), weight.reshape(OWNERS, COMP_DEV, W)))
    return (weighted.reshape(COMPLETIONS, W, D), advantages)
```

```python
import functools
import jax
import jax.numpy as jnp
from jax import lax
from jax.experimental import pallas as pl
from jax.experimental.pallas import tpu as pltpu
from jax.sharding import PartitionSpec as P

G = 16
AXES = ("gx", "gy", "gz")
STAGES = ("gz", "gx", "gy")
LANES = 128
norm_eps = 1e-05


def pack_body(cap, groups, prompt_ref, length_ref, gain_ref, rows_ref, out_ref,
              rows, wide, tokens, src, dst, count, first, in_sems, out_sem):
    total, pieces = rows.shape[0], in_sems.shape[0]
    piece = total // pieces
    half = wide.shape[1] // 2
    features = half * LANES
    for k in range(pieces):
        part = pl.ds(k * piece, piece)
        pltpu.make_async_copy(rows_ref.at[part], rows.at[part], in_sems.at[k]).start()

    def clear(o, _):
        count[o] = 0
        return 0
    lax.fori_loop(0, count.shape[0], clear, 0)

    def place(i, _):
        o = prompt_ref[i] // groups
        at = count[o]
        two = length_ref[i] > 1
        count[o] = at + jnp.where(two, 2, 1)
        base = o * cap

        @pl.when(at == 0)
        def _():
            first[o] = 2 * i
        head = first[o]
        ok0 = at < cap
        src[2 * i] = jnp.where(ok0, 2 * i, head)
        dst[2 * i] = base + jnp.where(ok0, at, 0)
        ok1 = two & (at + 1 < cap)
        src[2 * i + 1] = jnp.where(ok1, 2 * i + 1, src[2 * i])
        dst[2 * i + 1] = jnp.where(ok1, base + at + 1, dst[2 * i])
        return 0
    lax.fori_loop(0, total, place, 0)

    gain = gain_ref[...]
    batch = wide.shape[0]

    def work(j, _):
        for b in range(batch):
            i = j * batch + b
            wide[b] = rows[i].astype(jnp.float32)
            for t in range(2):
                x = wide[b, pl.ds(t, half, stride=2), :]
                s = jnp.sum(jnp.sum((x * x).reshape(half // 8, 8, LANES), axis=0), axis=1, keepdims=True)
                s = jnp.sum(s, axis=0, keepdims=True)
                r = lax.rsqrt(s * (1.0 / features) + norm_eps)
                tokens[2 * i + t] = (x * r * gain).astype(jnp.bfloat16)
        return 0

    def send(i, _):
        pltpu.make_async_copy(tokens.at[src[i]], out_ref.at[dst[i]], out_sem).start()
        return 0

    for k in range(pieces):
        part = pl.ds(k * piece, piece)
        pltpu.make_async_copy(rows_ref.at[part], rows.at[part], in_sems.at[k]).wait()
        lax.fori_loop(k * (piece // batch), (k + 1) * (piece // batch), work, 0)
        lax.fori_loop(k * 2 * piece, (k + 1) * 2 * piece, send, 0, unroll=8)
    pltpu.make_async_copy(tokens, tokens, out_sem).wait()


def unpack_body(slot_ref, weight_ref, tokens_ref, out_ref, tokens, wide, out, in_sem, out_sems):
    total, pieces = out.shape[0], out_sems.shape[0]
    piece = total // pieces
    half = wide.shape[1] // 2
    batch = wide.shape[0]
    pltpu.make_async_copy(tokens_ref, tokens, in_sem).start()
    pltpu.make_async_copy(tokens_ref, tokens, in_sem).wait()

    def work(j, _):
        for b in range(batch):
            i = j * batch + b
            for t in range(2):
                x = tokens[slot_ref[2 * i + t]].astype(jnp.float32)
                wide[b, pl.ds(t, half, stride=2), :] = x * weight_ref[2 * i + t]
            out[i] = wide[b].astype(jnp.bfloat16)
        return 0

    for k in range(pieces):
        part = pl.ds(k * piece, piece)
        lax.fori_loop(k * (piece // batch), (k + 1) * (piece // batch), work, 0)
        pltpu.make_async_copy(out.at[part], out_ref.at[part], out_sems.at[k]).start()
    for k in range(pieces):
        part = pl.ds(k * piece, piece)
        pltpu.make_async_copy(out.at[part], out_ref.at[part], out_sems.at[k]).wait()


def pack(rows, gain, prompt_of, lengths, owners, cap, groups):
    total, width, _ = rows.shape
    half = width // 2
    smem, vmem = pl.BlockSpec(memory_space=pltpu.SMEM), pl.BlockSpec(memory_space=pltpu.VMEM)
    return pl.pallas_call(
        functools.partial(pack_body, cap, groups),
        out_shape=jax.ShapeDtypeStruct((owners * cap, half, LANES), jnp.bfloat16),
        in_specs=[smem, smem, vmem, pl.BlockSpec(memory_space=pl.ANY)],
        out_specs=pl.BlockSpec(memory_space=pl.ANY),
        scratch_shapes=[
            pltpu.VMEM(rows.shape, jnp.bfloat16),
            pltpu.VMEM((4, width, LANES), jnp.float32),
            pltpu.VMEM((2 * total, half, LANES), jnp.bfloat16),
            pltpu.SMEM((2 * total,), jnp.int32),
            pltpu.SMEM((2 * total,), jnp.int32),
            pltpu.SMEM((owners,), jnp.int32),
            pltpu.SMEM((owners,), jnp.int32),
            pltpu.SemaphoreType.DMA((8,)),
            pltpu.SemaphoreType.DMA,
        ],
        name="pack",
    )(prompt_of, lengths, gain, rows)


def unpack(slots, weights, tokens, total):
    count, half, _ = tokens.shape
    smem, hbm = pl.BlockSpec(memory_space=pltpu.SMEM), pl.BlockSpec(memory_space=pl.ANY)
    return pl.pallas_call(
        unpack_body,
        out_shape=jax.ShapeDtypeStruct((total, 2 * half, LANES), jnp.bfloat16),
        in_specs=[smem, smem, hbm],
        out_specs=hbm,
        scratch_shapes=[
            pltpu.VMEM(tokens.shape, jnp.bfloat16),
            pltpu.VMEM((4, 2 * half, LANES), jnp.float32),
            pltpu.VMEM((total, 2 * half, LANES), jnp.bfloat16),
            pltpu.SemaphoreType.DMA,
            pltpu.SemaphoreType.DMA((8,)),
        ],
        name="unpack",
    )(slots, weights, tokens)


def partner(size, index, step):
    return index ^ step if size & (size - 1) == 0 else (index + step) % size


def origin(size, index, step):
    return index ^ step if size & (size - 1) == 0 else (index + size - step) % size


def on_device(hidden, norm_gain, prompt_of, lengths, reward_level):
    count_here, window, features = hidden.shape
    sizes = {a: lax.axis_size(a) for a in AXES}
    owners = sizes["gx"] * sizes["gy"] * sizes["gz"]
    slot_count = max(2, count_here // owners + 1)
    cap = window * slot_count
    groups = count_here // G
    half = features // LANES
    coord = {a: lax.axis_index(a) for a in AXES}
    me = (coord["gx"] * sizes["gy"] + coord["gy"]) * sizes["gz"] + coord["gz"]

    rows = hidden.reshape(count_here, window, half, LANES).transpose(0, 2, 1, 3)
    rows = rows.reshape(count_here, window * half, LANES)
    sent = pack(rows, norm_gain.reshape(half, LANES), prompt_of, lengths, owners, cap, groups)
    came = lax.all_to_all(sent, AXES, split_axis=0, concat_axis=0, tiled=True)

    known = jnp.stack([prompt_of, lengths, reward_level])[None]
    source = me[None]
    weight_of = {"gx": sizes["gy"] * sizes["gz"], "gy": sizes["gz"], "gz": 1}
    for a in STAGES:
        blocks, ids = [known], [source]
        for k in range(1, sizes[a]):
            pairs = [(i, partner(sizes[a], i, k)) for i in range(sizes[a])]
            blocks.append(lax.ppermute(known, a, pairs))
            ids.append(source + (origin(sizes[a], coord[a], k) - coord[a]) * weight_of[a])
        known, source = jnp.concatenate(blocks), jnp.concatenate(ids)

    f32 = jnp.float32
    prompts, lens, levels = known[:, 0], known[:, 1], known[:, 2]
    mine = prompts // groups == me
    spot = jnp.arange(count_here)
    before = (spot[:, None] < spot[None, :]).astype(f32)
    group = jnp.arange(groups)
    same = (prompts[None] == me * groups + group[:, None, None]).astype(f32)
    within = jnp.einsum("gsj,jk->gsk", same, before, preferred_element_type=f32)
    earlier = (source[:, None] < source[None, :]).astype(f32)
    ahead = jnp.einsum("gs,sr->gr", jnp.sum(same, axis=2), earlier, precision=lax.Precision.HIGHEST)
    target = jnp.sum(same * (within + ahead[:, :, None] + (G * group + 1).astype(f32)[:, None, None]), axis=0) - 1
    live = jnp.where(mine, lens, 0)
    at = jnp.dot(live.astype(f32), before, preferred_element_type=f32).astype(jnp.int32)
    code = ((source[:, None] * cap + at) * 16 + levels) * 4 + lens
    hit = target.astype(jnp.int32)[None] == spot[:, None, None]
    code = jnp.sum(jnp.where(hit, code[None], 0), axis=(1, 2))
    size, level, slot = code % 4, (code // 4) % 16, code // 64

    levels = level.astype(f32).reshape(groups, G)
    average = jnp.mean(levels, axis=1, keepdims=True)
    centered = levels - average
    spread = jnp.sqrt(jnp.mean(centered * centered, axis=1, keepdims=True))
    advantages = (centered / jnp.maximum(spread, 1.0)).reshape(count_here)
    t = jnp.arange(window)
    alive = t[None, :] < size[:, None]
    weight = jnp.where(alive, advantages[:, None] / size[:, None].astype(f32), 0.0)
    slots = slot[:, None] + jnp.where(alive, t[None, :], 0)
    out = unpack(slots.reshape(-1), weight.reshape(-1), came, count_here)
    out = out.reshape(count_here, half, window, LANES).transpose(0, 2, 1, 3)
    return out.reshape(count_here, window, features), advantages


def solution(mesh):
    many = P(AXES)
    return jax.shard_map(
        on_device, mesh=mesh,
        in_specs=(P(AXES, None, None), P(), many, many, many),
        out_specs=(P(AXES, None, None), many), check_vma=False,
    )
```

```python
import functools
import jax
import numpy as np
import jax.numpy as jnp
from jax import lax
from jax.experimental import pallas as pl
from jax.experimental.pallas import tpu as pltpu
from jax.sharding import PartitionSpec as P

G = 16
AXES = ("gx", "gy", "gz")
STAGES = ("gz", "gx", "gy")
LANES = 128
BATCH = 4
norm_eps = 1e-05


def pack_body(cap, slots, groups, prompt_ref, length_ref, level_ref, gain_ref, rows_ref,
              out_ref, spill_ref, table_ref, code_ref,
              rows, wide, tokens, src, dst, count, first, in_sems, out_sem):
    total, pieces = rows.shape[0], in_sems.shape[0]
    piece = total // pieces
    batch = wide.shape[0]
    half = wide.shape[1] // 2
    features = half * LANES
    limit = spill_ref.shape[0]
    owners = count.shape[0]
    for k in range(pieces):
        part = pl.ds(k * piece, piece)
        pltpu.make_async_copy(rows_ref.at[part], rows.at[part], in_sems.at[k]).start()

    for o in range(count.shape[0]):
        count[o] = 0
        first[o] = 0
    for e in range(table_ref.shape[0]):
        table_ref[e] = 0
    for e in range(code_ref.shape[0]):
        code_ref[e] = 0
    gain = gain_ref[...]

    def place(i, spilled):
        p = prompt_ref[i]
        n = length_ref[i]
        o = lax.div(p, groups)
        held = count[o]
        at, nth = held & 255, held >> 8
        count[o] = held + 256 + n
        field = nth * owners + o
        table_ref[field] = p - o * groups + 1
        table_ref[field + slots * owners] = n
        table_ref[field + 2 * slots * owners] = level_ref[i]
        base = o * cap
        head = jnp.where(at == 0, 2 * i, first[o])
        first[o] = head
        ok0 = at < cap
        s0 = jnp.where(ok0, 2 * i, head)
        d0 = base + jnp.where(ok0, at, 0)
        two = n > 1
        ok1 = two & (at + 1 < cap)
        src[2 * i], dst[2 * i] = s0, d0
        src[2 * i + 1] = jnp.where(ok1, 2 * i + 1, s0)
        dst[2 * i + 1] = jnp.where(ok1, d0 + 1, d0)
        if code_ref.shape[0] > limit:
            mark = (o * 256 + at) * 1024
            code_ref[jnp.minimum(spilled, limit)] = mark + 2 * i + 1
            spilled = spilled + jnp.where(ok0, 0, 1)
            code_ref[jnp.minimum(spilled, limit)] = mark + 1024 + 2 * i + 2
            spilled = spilled + jnp.where(two & (at + 1 >= cap), 1, 0)
        return spilled

    def send(i):
        pltpu.make_async_copy(tokens.at[src[i]], out_ref.at[dst[i]], out_sem).start()

    def work(j):
        for b in range(batch):
            i = j * batch + b
            wide[b] = rows[i].astype(jnp.float32)
        for b in range(batch):
            i = j * batch + b
            for t in range(2):
                x = wide[b, pl.ds(t, half, stride=2), :]
                s = jnp.sum((x * x).reshape(half // 8, 8, LANES), axis=0)
                s = jnp.sum(jnp.sum(s, axis=1, keepdims=True), axis=0, keepdims=True)
                r = lax.rsqrt(s * (1.0 / features) + norm_eps)
                tokens[2 * i + t] = (x * r * gain).astype(jnp.bfloat16)

    def step(j, spilled):
        for b in range(2 * batch):
            send((j - 1) * 2 * batch + b)
        for b in range(batch):
            spilled = place(j * batch + b, spilled)
        work(j)
        return spilled

    per = piece // batch

    def load(k):
        part = pl.ds(k * piece, piece)
        pltpu.make_async_copy(rows_ref.at[part], rows.at[part], in_sems.at[k]).wait()

    def chunk(k, spilled):
        load(k)
        return lax.fori_loop(k * per, (k + 1) * per, step, spilled)

    spilled = jnp.int32(0)
    for b in range(batch):
        spilled = place(b, spilled)
    load(0)
    work(0)
    spilled = lax.fori_loop(1, per, step, spilled)
    spilled = lax.fori_loop(1, pieces, chunk, spilled)
    for b in range(2 * batch):
        send(2 * (total - batch) + b)
    for o in range(owners):
        table_ref[3 * slots * owners + o] = jnp.maximum((count[o] & 255) - cap, 0)
    if code_ref.shape[0] > limit:
        for e in range(limit):
            code = jnp.where(e < spilled, code_ref[e], 0)
            code_ref[e] = code
            spill_ref[e] = tokens[jnp.maximum((code & 1023) - 1, 0)]
    else:
        spill_ref[...] = jnp.zeros(spill_ref.shape, spill_ref.dtype)
    pltpu.make_async_copy(rows_ref, rows, out_sem).wait()


def select(parts, near_axes, axis, room, spot_ref, shape):
    f32 = jnp.float32
    size, stride, mine = axis
    moved, offset = None, jnp.zeros((1, LANES), f32)
    for ref in parts:
        p = ref.shape[0]
        info = ref[:, shape[0]:shape[0] + LANES].astype(f32)
        dest = info[:, 1:2].astype(jnp.int32)
        lane = lax.broadcasted_iota(jnp.int32, (p, LANES), 1)
        go = (lane < (size - 1) * room) & (info[:, 0:1] > 0)
        for n, st, at in near_axes:
            go = go & (((dest >> st) & (n - 1)) == spot_ref[at])
        turn = lane & (room - 1)
        to = spot_ref[mine] ^ ((lane >> (room.bit_length() - 1)) + 1)
        go = jnp.where(go & (((dest >> stride) & (size - 1)) == to), 1.0, 0.0)
        row = lax.broadcasted_iota(jnp.int32, (p, p), 0)
        col = lax.broadcasted_iota(jnp.int32, (p, p), 1)
        nth = jnp.dot(jnp.where(col < row, 1.0, 0.0), go, preferred_element_type=f32) + offset
        offset = offset + jnp.sum(go, axis=0, keepdims=True)
        pick = jnp.where(nth == turn.astype(f32), go, 0.0)[:, :(size - 1) * room]
        data = ref[:, :shape[0] + LANES].astype(f32)
        part = lax.dot_general(pick, data, (((0,), (0,)), ((), ())), preferred_element_type=f32)
        moved = part if moved is None else moved + part
    return moved


def crowding(known, owners, fields, near_axes, axis, room, spot_ref):
    f32 = jnp.float32
    size, stride, mine = axis
    o = lax.broadcasted_iota(jnp.int32, (owners, LANES), 0)
    b = lax.broadcasted_iota(jnp.int32, (owners, LANES), 1)
    at = (o >> stride) & (size - 1)
    place = at
    span = size
    for n, st, _ in near_axes:
        place = place + span * ((o >> st) & (n - 1))
        span *= n
    member = jnp.where((place == b) & (at != spot_ref[mine]), 1.0, 0.0)
    total = jnp.zeros((1, LANES), f32)
    for k in known:
        left = jnp.sum(k[:, fields - owners:fields], axis=0, keepdims=True)
        total = total + jnp.dot(left, member, preferred_element_type=f32)
    return jnp.max(jnp.where(total > room, 1.0, 0.0), axis=1, keepdims=True)


def first_body(near_axes, axis, room, owners, fields, spot_ref, code_ref, table_ref, spill_ref, hold_ref, send_ref, table, wide, sem):
    f32 = jnp.float32
    limit, half, _ = spill_ref.shape
    features = half * LANES
    fetch = pltpu.make_async_copy(table_ref, table, sem)
    fetch.start()
    wide[...] = spill_ref[...].astype(f32)
    for c in range(half):
        hold_ref[:, c * LANES:(c + 1) * LANES] = wide[:, c, :].astype(jnp.bfloat16)
    row = lax.broadcasted_iota(jnp.int32, (limit, LANES), 0)
    lane = lax.broadcasted_iota(jnp.int32, (limit, LANES), 1)
    info = jnp.zeros((limit, LANES), jnp.int32)
    for e in range(limit):
        code = code_ref[e]
        used = jnp.where(code > 0, 1, 0)
        mark = code >> 10
        value = jnp.where(lane == 0, used, jnp.where(lane == 1, mark >> 8, jnp.where(lane == 2, spot_ref[3], jnp.where(lane == 3, mark & 255, 0))))
        info = jnp.where((row == e) & (code > 0), value, info)
    hold_ref[:, features:features + LANES] = info.astype(f32).astype(jnp.bfloat16)
    fetch.wait()
    width = table.shape[0] * LANES
    own = jnp.concatenate([table[r:r + 1, :] for r in range(table.shape[0])], axis=1).astype(f32)
    first = lax.broadcasted_iota(jnp.int32, (limit, width), 0) == 0
    known = jnp.where(first, own, 0.0)
    hold_ref[:, features + LANES:] = known.astype(jnp.bfloat16)
    left = jnp.sum(own[:, fields - owners:fields], axis=1, keepdims=True)
    bad = jnp.where(left > limit, 1.0, 0.0)
    bad = jnp.maximum(bad, crowding([known], owners, fields, near_axes, axis, room, spot_ref))
    moved = select([hold_ref], near_axes, axis, room, spot_ref, (features,))
    finish(moved, [known], bad, room, features, send_ref)


def finish(moved, known, bad, room, features, send_ref):
    rows = moved.shape[0]
    lane = lax.broadcasted_iota(jnp.int32, (rows, LANES), 1)
    info = jnp.where(lane == 4, bad, jnp.where(lane < 4, moved[:, features:], 0.0))
    for k in range(send_ref.shape[0]):
        part = slice(k * room, (k + 1) * room)
        send_ref[k, :, :features] = moved[part, :features].astype(jnp.bfloat16)
        send_ref[k, :, features:features + LANES] = info[part].astype(jnp.bfloat16)
        at = features + LANES
        for v in known:
            send_ref[k, :, at:at + v.shape[1]] = v.astype(jnp.bfloat16)
            at += v.shape[1]


def next_body(near_axes, axis, room, owners, fields, width, count, features, parts, recent, spot_ref, *refs):
    f32 = jnp.float32
    holds, own_ref, send_ref = refs[:parts], refs[parts], refs[parts + 1]
    came = holds[parts - recent:]
    at = features + LANES
    blocks = (own_ref.shape[1] - at) // width
    bad = None
    known = []
    for i, ref in enumerate((own_ref, *came)):
        flag = jnp.max(ref[:, features:features + LANES].astype(f32)[:, 4:5], axis=0, keepdims=True)
        bad = flag if bad is None else jnp.maximum(bad, flag)
        for j in range(blocks):
            value = ref[:, at + j * width:at + (j + 1) * width].astype(f32)
            if count >= room:
                known.append(value)
                continue
            rows = ref.shape[0]
            to = lax.broadcasted_iota(jnp.int32, (room, rows), 0)
            source = lax.broadcasted_iota(jnp.int32, (room, rows), 1)
            shift = (i * count) % room
            put = jnp.where((to == source + shift) & (source < count), 1.0, 0.0)
            value = jnp.dot(put, value, preferred_element_type=f32)
            if (i * count) // room == len(known):
                known.append(value)
            else:
                known[-1] = known[-1] + value
    bad = jnp.maximum(bad, crowding(known, owners, fields, near_axes, axis, room, spot_ref))
    moved = select(holds, near_axes, axis, room, spot_ref, (features,))
    finish(moved, known, bad, room, features, send_ref)


def final_body(cap, slots, owners, fields, width, features, groups, parts, spot_ref, id_col_ref, id_row_ref, tokens_ref, *refs):
    f32, i32 = jnp.float32, jnp.int32
    known_refs, holds = refs[:parts[0]], refs[parts[0]:parts[0] + parts[1]]
    out_ref, adv_ref, tokens, wide, out, extra, slot_v, weight_v, slot_s, weight_s, in_sem, table_sems, out_sems = refs[parts[0] + parts[1]:]
    total, pieces = out.shape[0], out_sems.shape[0]
    main = tokens_ref.shape[0]
    half = features // LANES
    fetch = pltpu.make_async_copy(tokens_ref, tokens.at[pl.ds(0, main)], in_sem)
    fetch.start()

    lane = lax.broadcasted_iota(i32, (width, LANES), 0)
    column = lax.broadcasted_iota(i32, (width, LANES), 1)
    mine = jnp.where(((lane >> (owners.bit_length() - 1)) == column) & ((lane & (owners - 1)) == spot_ref[3]) & (lane < fields - owners), 1.0, 0.0)
    entry = []
    for ref in known_refs:
        for j in range((ref.shape[1] - features - LANES) // width):
            at = features + LANES + j * width
            entry.append(jnp.dot(ref[:, at:at + width].astype(f32), mine, preferred_element_type=f32))
    entry = jnp.concatenate(entry, axis=0)
    turned = entry.T
    ids, ids_row = id_col_ref[...], id_row_ref[...]
    label = [entry[:, k:k + 1] for k in range(slots)]
    size = [entry[:, slots + k:slots + k + 1] for k in range(slots)]
    level = [entry[:, 2 * slots + k:2 * slots + k + 1] for k in range(slots)]
    if holds:
        info = jnp.concatenate([ref[:, features:features + LANES].astype(f32) for ref in holds], axis=0)
        there = info.T
        key = jnp.where((there[0:1] > 0) & (there[1:2] == spot_ref[3].astype(f32)), there[2:3] * 256.0 + there[3:4], -1.0)
        held_at = lax.broadcasted_iota(i32, (owners, key.shape[1]), 1).astype(f32)
    q = lax.broadcasted_iota(i32, (owners, total), 1).astype(f32)
    rows = [jnp.zeros((1, total), f32) for _ in range(4)]
    pos = jnp.zeros((owners, 1), f32)
    for k in range(slots):
        rank = jnp.zeros((owners, owners), f32)
        for j in range(slots):
            ahead = (ids_row < ids) if j >= k else (ids_row <= ids)
            rank = rank + jnp.where((label[k] == turned[j:j + 1, :]) & ahead, 1.0, 0.0)
        target = jnp.where(label[k] > 0, (label[k] - 1.0) * G + jnp.sum(rank, axis=1, keepdims=True), -1.0)
        places = []
        for t in range(2):
            p = pos if t == 0 else pos + jnp.where(size[k] > 1, 1.0, 0.0)
            place = ids * cap + p
            if holds:
                hit = jnp.where(key == ids * 256.0 + p, held_at, 0.0)
                place = jnp.where(p < cap, place, main + jnp.sum(hit, axis=1, keepdims=True))
            places.append(place)
        hit = target == q
        for r, v in enumerate((*places, size[k], level[k])):
            rows[r] = rows[r] + jnp.sum(jnp.where(hit, v, 0.0), axis=0, keepdims=True)
        pos = pos + size[k]
    slot_v[0:1, :] = rows[0].astype(i32)
    slot_v[1:2, :] = rows[1].astype(i32)
    n, lv = rows[2], rows[3]
    a = lax.broadcasted_iota(i32, (total, total), 0) // G
    b = lax.broadcasted_iota(i32, (total, total), 1) // G
    group = jnp.where(a == b, 1.0, 0.0)
    mean = jnp.dot(lv, group, preferred_element_type=f32) * (1.0 / G)
    square = jnp.dot(lv * lv, group, preferred_element_type=f32) * (1.0 / G)
    spread = jnp.sqrt(square - mean * mean)
    advantage = (lv - mean) / jnp.maximum(spread, 1.0)
    adv_ref[...] = advantage
    weight_v[0:1, :] = advantage / n
    weight_v[1:2, :] = jnp.where(n > 1, advantage / n, 0.0)
    copy_slot = pltpu.make_async_copy(slot_v, slot_s, table_sems.at[0])
    copy_weight = pltpu.make_async_copy(weight_v, weight_s, table_sems.at[1])
    copy_slot.start()
    copy_weight.start()
    base = 0
    for ref in holds:
        p = ref.shape[0]
        for c in range(half):
            extra[base:base + p, c, :] = ref[:, c * LANES:(c + 1) * LANES].astype(f32)
        base += p
    for h in range(base):
        tokens[main + h] = extra[h].astype(jnp.bfloat16)
    copy_slot.wait()
    copy_weight.wait()
    fetch.wait()

    batch = wide.shape[0]
    piece = total // pieces

    def work(j, _):
        for e in range(batch):
            i = j * batch + e
            for t in range(2):
                x = tokens[slot_s[t, i]].astype(f32)
                wide[e, pl.ds(t, half, stride=2), :] = x * weight_s[t, i]
        for e in range(batch):
            out[j * batch + e] = wide[e].astype(jnp.bfloat16)
        return 0

    def chunk(k, _):
        lax.fori_loop(k * (piece // batch), (k + 1) * (piece // batch), work, 0)
        part = pl.ds(k * piece, piece)
        pltpu.make_async_copy(out.at[part], out_ref.at[part], out_sems.at[k]).start()
        return 0
    lax.fori_loop(0, pieces, chunk, 0)
    for k in range(pieces):
        part = pl.ds(k * piece, piece)
        pltpu.make_async_copy(out.at[part], out_ref.at[part], out_sems.at[k]).wait()


SMEM = pl.BlockSpec(memory_space=pltpu.SMEM)
VMEM = pl.BlockSpec(memory_space=pltpu.VMEM)
HBM = pl.BlockSpec(memory_space=pl.ANY)
COST = pl.CostEstimate(flops=1 << 20, bytes_accessed=1 << 20, transcendentals=0)


def pack(rows, gain, prompt_of, lengths, levels, owners, cap, slots, groups, limit, words):
    total, width, _ = rows.shape
    half = width // 2
    return pl.pallas_call(
        functools.partial(pack_body, cap, slots, groups),
        out_shape=[
            jax.ShapeDtypeStruct((owners * cap, half, LANES), jnp.bfloat16),
            jax.ShapeDtypeStruct((max(limit, 1), half, LANES), jnp.bfloat16),
            jax.ShapeDtypeStruct((words,), jnp.int32),
            jax.ShapeDtypeStruct((limit + 1,), jnp.int32),
        ],
        in_specs=[SMEM, SMEM, SMEM, VMEM, HBM],
        out_specs=[HBM, VMEM, SMEM, SMEM],
        scratch_shapes=[
            pltpu.VMEM(rows.shape, jnp.bfloat16),
            pltpu.VMEM((BATCH, width, LANES), jnp.float32),
            pltpu.VMEM((2 * total, half, LANES), jnp.bfloat16),
            pltpu.SMEM((2 * total,), jnp.int32),
            pltpu.SMEM((2 * total,), jnp.int32),
            pltpu.SMEM((owners,), jnp.int32),
            pltpu.SMEM((owners,), jnp.int32),
            pltpu.SemaphoreType.DMA((8,)),
            pltpu.SemaphoreType.DMA,
        ],
        cost_estimate=COST,
        name="pack",
    )(prompt_of, lengths, levels, gain, rows)


def partner(size, index, step):
    return index ^ step


def log2(n):
    assert n & (n - 1) == 0
    return n.bit_length() - 1


def on_device(hidden, norm_gain, prompt_of, lengths, reward_level):
    f32, i32, bf16 = jnp.float32, jnp.int32, jnp.bfloat16
    count_here, window, features = hidden.shape
    sizes = {a: lax.axis_size(a) for a in AXES}
    owners = sizes["gx"] * sizes["gy"] * sizes["gz"]
    slots = max(2, count_here // owners + 1)
    mean = window * count_here // owners
    full = window * slots
    cap = min(full, max(window, mean - mean // 8))
    limit = 16
    room = {STAGES[0]: limit if (sizes[STAGES[0]] - 1) * limit <= LANES else 8, STAGES[1]: 8, STAGES[2]: 8}
    groups = count_here // G
    half = features // LANES
    stride = {"gx": sizes["gy"] * sizes["gz"], "gy": sizes["gz"], "gz": 1}
    spot_at = {"gx": 0, "gy": 1, "gz": 2}
    coord = {a: lax.axis_index(a) for a in AXES}
    me = sum(coord[a] * stride[a] for a in AXES)
    spot = jnp.stack([coord["gx"], coord["gy"], coord["gz"], me]).astype(i32)
    fields = 3 * slots * owners + owners
    width = -(-fields // LANES) * LANES

    rows = hidden.reshape(count_here, window, half, LANES).transpose(0, 2, 1, 3)
    rows = rows.reshape(count_here, window * half, LANES)
    gain = norm_gain.reshape(half, LANES)
    sent, spill, table, codes = pack(rows, gain, prompt_of, lengths, reward_level, owners, cap, slots, groups, limit, width)
    with jax.named_scope("exchange"):
        came = lax.all_to_all(sent, AXES, split_axis=0, concat_axis=0, tiled=True)

    def axis(a):
        return sizes[a], log2(stride[a]), spot_at[a]

    lanes = features + LANES
    holds, got, own, near, count = [], [], None, [], 1
    steps = {x: np.zeros((1,), np.int32) for x in AXES}
    for n, a in enumerate(STAGES):
        size = sizes[a]
        shape = functools.partial(jax.ShapeDtypeStruct, dtype=bf16)
        with jax.named_scope("stage" + str(n)):
            if n == 0:
                hold, send = pl.pallas_call(
                    functools.partial(first_body, tuple(near), axis(a), room[a], owners, fields),
                    out_shape=[shape((limit, lanes + width)), shape((size - 1, room[a], lanes + width))],
                    in_specs=[SMEM, SMEM, SMEM, VMEM], out_specs=[VMEM, VMEM],
                    scratch_shapes=[pltpu.VMEM((width // LANES, LANES), i32), pltpu.VMEM((limit, half, LANES), f32), pltpu.SemaphoreType.DMA],
                    cost_estimate=COST, name="stage",
                )(spot, codes, table.reshape(width // LANES, LANES), spill)
                holds = [hold]
            else:
                blocks = -(-count // room[a])
                send = pl.pallas_call(
                    functools.partial(next_body, tuple(near), axis(a), room[a], owners, fields, width, before, features, len(holds), len(got)),
                    out_shape=shape((size - 1, room[a], lanes + blocks * width)),
                    in_specs=[SMEM] + [VMEM] * (len(holds) + 1), out_specs=VMEM,
                    cost_estimate=COST, name="stage",
                )(spot, *holds, own)
            got = []
            for k in range(1, size):
                pairs = [(i, partner(size, i, k)) for i in range(size)]
                got.append(lax.ppermute(send[k - 1], a, pairs))
            own = send[0]
            holds = holds + got
        near.append(axis(a))
        before = count
        count *= size
        order = np.arange(size, dtype=np.int32)
        steps = {x: np.concatenate([v + (k if x == a else 0) for k in order]) for x, v in steps.items()}

    ids = sum((coord[a] ^ steps[a]) * stride[a] for a in AXES).astype(f32)
    known = [own, *got]
    bad = jnp.max(jnp.stack([v[0, features + 4] for v in known])) > 0

    def finish_with(tokens, cap_used, extras):
        spare = sum(h.shape[0] for h in extras)
        out, advantages = pl.pallas_call(
            functools.partial(final_body, cap_used, slots, owners, fields, width, features, groups, (len(known), len(extras))),
            out_shape=[jax.ShapeDtypeStruct((count_here, window * half, LANES), bf16), jax.ShapeDtypeStruct((1, count_here), f32)],
            in_specs=[SMEM, VMEM, VMEM, HBM] + [VMEM] * (len(known) + len(extras)), out_specs=[HBM, VMEM],
            scratch_shapes=[
                pltpu.VMEM((tokens.shape[0] + spare, half, LANES), bf16),
                pltpu.VMEM((4, window * half, LANES), f32),
                pltpu.VMEM((count_here, window * half, LANES), bf16),
                pltpu.VMEM((max(spare, 8), half, LANES), f32),
                pltpu.VMEM((window, count_here), i32),
                pltpu.VMEM((window, count_here), f32),
                pltpu.SMEM((window, count_here), i32),
                pltpu.SMEM((window, count_here), f32),
                pltpu.SemaphoreType.DMA,
                pltpu.SemaphoreType.DMA((2,)),
                pltpu.SemaphoreType.DMA((8,)),
            ],
            cost_estimate=COST, name="place",
        )(spot, ids[:, None], ids[None], tokens, *known, *extras)
        out = out.reshape(count_here, half, window, LANES).transpose(0, 2, 1, 3)
        return out.reshape(count_here, window, features), advantages.reshape(count_here)

    def usual():
        return finish_with(came, cap, holds)

    def crowded():
        again = pack(rows, gain, prompt_of, lengths, reward_level, owners, full, slots, groups, 0, width)
        all_came = lax.all_to_all(again[0], AXES, split_axis=0, concat_axis=0, tiled=True)
        return finish_with(all_came, full, [])
    return lax.cond(bad, crowded, usual)


def solution(mesh):
    many = P(AXES)
    return jax.shard_map(
        on_device, mesh=mesh,
        in_specs=(P(AXES, None, None), P(), many, many, many),
        out_specs=(P(AXES, None, None), many), check_vma=False,
    )
```

```python
import functools
import jax
import numpy as np
import jax.numpy as jnp
from jax import lax
from jax.experimental import pallas as pl
from jax.experimental.pallas import tpu as pltpu
from jax.sharding import PartitionSpec as P

G = 16
AXES = ("gx", "gy", "gz")
LANES = 128
BATCH = 16
norm_eps = 1e-05


def pack_body(cap, groups, limit, spot_ref, prompt_ref, length_ref, gain_ref, rows_ref,
              out_ref, spill_ref, mark_ref, nth_ref,
              rows, wide, tokens, way_v, list_v, way, spilled, in_sems, way_sems):
    f32, i32 = jnp.float32, jnp.int32
    total, pieces = rows.shape[0], in_sems.shape[0]
    piece = total // pieces
    batch = wide.shape[0]
    half = wide.shape[1] // 2
    features = half * LANES
    for k in range(pieces):
        part = pl.ds(k * piece, piece)
        pltpu.make_async_copy(rows_ref.at[part], rows.at[part], in_sems.at[k]).start()

    p, n = prompt_ref[...], length_ref[...]
    column = jnp.broadcast_to((p * 4 + n).astype(f32), (total, total)).T.astype(i32)
    before = lax.broadcasted_iota(i32, (total, total), 0) < lax.broadcasted_iota(i32, (total, total), 1)
    owner = p >> log2(groups)
    same = ((column >> (2 + log2(groups))) == owner) & before
    at = jnp.sum(jnp.where(same, column & 3, 0), axis=0, keepdims=True)
    nth_ref[...] = jnp.sum(jnp.where(same, 1, 0), axis=0, keepdims=True)
    lane = lax.broadcasted_iota(i32, (1, total), 1)
    home = jnp.sum(jnp.where(lane == 0, owner, 0), axis=1, keepdims=True) * cap
    d0 = jnp.where(at < cap, owner * cap + at, home)
    way_v[0:1, :] = d0
    way_v[1:2, :] = jnp.where((n > 1) & (at + 1 < cap), d0 + 1, d0)
    pltpu.make_async_copy(way_v, way, way_sems.at[0]).start()
    if limit:
        over = jnp.where(at >= cap, 1, 0)
        more = jnp.where((n > 1) & (at + 1 >= cap), 1, 0)
        start = jnp.dot((over + more).astype(f32), jnp.where(before, 1.0, 0.0), preferred_element_type=f32).astype(i32)
        e = lax.broadcasted_iota(i32, (limit, total), 0)
        hit0 = (over > 0) & (start == e)
        hit1 = (more > 0) & (start + over == e)
        token = jnp.sum(jnp.where(hit0, 2 * lane + 1, jnp.where(hit1, 2 * lane + 2, 0)), axis=1, keepdims=True)
        dest = jnp.sum(jnp.where(hit0 | hit1, owner, 0), axis=1, keepdims=True)
        spot = jnp.sum(jnp.where(hit0, at, jnp.where(hit1, at + 1, 0)), axis=1, keepdims=True)
        lanes = lax.broadcasted_iota(i32, (limit, LANES), 1)
        mark = jnp.where(lanes == 0, 1, jnp.where(lanes == 1, dest, jnp.where(lanes == 2, spot_ref[0], jnp.where(lanes == 3, spot, 0))))
        mark_ref[...] = jnp.where(token > 0, mark, 0).astype(f32).astype(jnp.bfloat16)
        list_v[...] = jnp.broadcast_to(jnp.maximum(token - 1, 0), list_v.shape)
        pltpu.make_async_copy(list_v, spilled, way_sems.at[1]).start()
    else:
        mark_ref[...] = jnp.zeros(mark_ref.shape, mark_ref.dtype)
    gain = gain_ref[...]
    pltpu.make_async_copy(way_v, way, way_sems.at[0]).wait()

    def work(j, _):
        for b in range(batch):
            wide[b] = rows[j * batch + b].astype(f32)
        for b in range(batch):
            i = j * batch + b
            for t in (1, 0):
                x = wide[b, pl.ds(t, half, stride=2), :]
                s = jnp.sum((x * x).reshape(half // 8, 8, LANES), axis=0)
                s = jnp.sum(jnp.sum(s, axis=1, keepdims=True), axis=0, keepdims=True)
                r = lax.rsqrt(s * (1.0 / features) + norm_eps)
                x = (x * r * gain).astype(jnp.bfloat16)
                out_ref[way[t, i]] = x
                tokens[2 * i + t] = x
        return 0

    per = piece // batch

    def chunk(k, _):
        part = pl.ds(k * piece, piece)
        pltpu.make_async_copy(rows_ref.at[part], rows.at[part], in_sems.at[k]).wait()
        return lax.fori_loop(k * per, (k + 1) * per, work, 0)
    lax.fori_loop(0, pieces, chunk, 0)
    out_ref[way[0, 0]] = tokens[0]
    if limit:
        pltpu.make_async_copy(list_v, spilled, way_sems.at[1]).wait()
        for e in range(limit):
            spill_ref[e] = tokens[spilled[e, 0]]
    else:
        spill_ref[...] = jnp.zeros(spill_ref.shape, spill_ref.dtype)


def select(parts, near_axes, axis, room, spot_ref, shape):
    f32 = jnp.float32
    size, stride, mine = axis
    moved, offset = None, jnp.zeros((1, LANES), f32)
    for ref in parts:
        p = ref.shape[0]
        info = ref[:, shape[0]:shape[0] + LANES].astype(f32)
        dest = info[:, 1:2].astype(jnp.int32)
        lane = lax.broadcasted_iota(jnp.int32, (p, LANES), 1)
        go = (lane < (size - 1) * room) & (info[:, 0:1] > 0)
        for n, st, at in near_axes:
            go = go & (((dest >> st) & (n - 1)) == spot_ref[at])
        turn = lane & (room - 1)
        to = spot_ref[mine] ^ ((lane >> (room.bit_length() - 1)) + 1)
        go = jnp.where(go & (((dest >> stride) & (size - 1)) == to), 1.0, 0.0)
        row = lax.broadcasted_iota(jnp.int32, (p, p), 0)
        col = lax.broadcasted_iota(jnp.int32, (p, p), 1)
        nth = jnp.dot(jnp.where(col < row, 1.0, 0.0), go, preferred_element_type=f32) + offset
        offset = offset + jnp.sum(go, axis=0, keepdims=True)
        pick = jnp.where(nth == turn.astype(f32), go, 0.0)[:, :(size - 1) * room]
        data = ref[:, :shape[0] + LANES].astype(f32)
        part = lax.dot_general(pick, data, (((0,), (0,)), ((), ())), preferred_element_type=f32)
        moved = part if moved is None else moved + part
    return moved


def crowding(known, owners, fields, near_axes, axis, room, spot_ref):
    f32 = jnp.float32
    size, stride, mine = axis
    o = lax.broadcasted_iota(jnp.int32, (owners, LANES), 0)
    b = lax.broadcasted_iota(jnp.int32, (owners, LANES), 1)
    at = (o >> stride) & (size - 1)
    place = at
    span = size
    for n, st, _ in near_axes:
        place = place + span * ((o >> st) & (n - 1))
        span *= n
    member = jnp.where((place == b) & (at != spot_ref[mine]), 1.0, 0.0)
    total = jnp.zeros((1, LANES), f32)
    for k in known:
        left = jnp.sum(k[:, fields - owners:fields], axis=0, keepdims=True)
        total = total + jnp.dot(left, member, preferred_element_type=f32)
    return jnp.max(jnp.where(total > room, 1.0, 0.0), axis=1, keepdims=True)


def first_body(near_axes, axis, room, owners, fields, width, cap, groups, spot_ref, prompt_ref, length_ref, level_ref, nth_ref, mark_ref, spill_ref, hold_ref, *rest):
    f32, i32 = jnp.float32, jnp.int32
    limit, half, _ = spill_ref.shape
    features = half * LANES
    send_refs, wide = rest[:-1], rest[-1]
    wide[...] = spill_ref[...].astype(f32)
    for c in range(half):
        hold_ref[:, c * LANES:(c + 1) * LANES] = wide[:, c, :].astype(jnp.bfloat16)
    hold_ref[:, features:features + LANES] = mark_ref[...]
    p, n = prompt_ref[...], length_ref[...]
    total = p.shape[1]
    owner = p >> log2(groups)
    place = nth_ref[...] * owners + owner
    column = jnp.broadcast_to(place.astype(f32), (total, total)).T.astype(i32)[:, :1]
    lane = lax.broadcasted_iota(i32, (total, width), 1)
    block = (fields - owners) // 3
    own = jnp.zeros((1, width), f32)
    for k, v in enumerate(((p & (groups - 1)) + 1, n, level_ref[...])):
        here = jnp.where(lane == column + k * block, 1.0, 0.0)
        own = own + jnp.dot(v.astype(f32), here, preferred_element_type=f32)
    here = jnp.where(lane == (column & (owners - 1)) + 3 * block, 1.0, 0.0)
    tokens = jnp.dot(n.astype(f32), here, preferred_element_type=f32)
    own = own + jnp.maximum(tokens - cap, 0.0)
    first = lax.broadcasted_iota(i32, (limit, width), 0) == 0
    known = jnp.where(first, own, 0.0)
    hold_ref[:, features + LANES:] = known.astype(jnp.bfloat16)
    left = jnp.sum(own[:, fields - owners:fields], axis=1, keepdims=True)
    bad = jnp.where(left > limit, 1.0, 0.0)
    bad = jnp.maximum(bad, crowding([known], owners, fields, near_axes, axis, room, spot_ref))
    moved = select([hold_ref], near_axes, axis, room, spot_ref, (features,))
    finish(moved, [known[:room]], bad, room, features, send_refs)


def finish(moved, known, bad, room, features, send_refs):
    rows = moved.shape[0]
    lane = lax.broadcasted_iota(jnp.int32, (rows, LANES), 1)
    info = jnp.where(lane == 4, bad, jnp.where(lane < 4, moved[:, features:], 0.0))
    for k, send_ref in enumerate(send_refs):
        part = slice(k * room, (k + 1) * room)
        send_ref[:, :features] = moved[part, :features].astype(jnp.bfloat16)
        send_ref[:, features:features + LANES] = info[part].astype(jnp.bfloat16)
        at = features + LANES
        for v in known:
            send_ref[:, at:at + v.shape[1]] = v.astype(jnp.bfloat16)
            at += v.shape[1]


def next_body(near_axes, axis, room, owners, fields, width, count, features, parts, recent, spot_ref, *refs):
    f32 = jnp.float32
    holds, own_ref, send_refs = refs[:parts], refs[parts], refs[parts + 1:]
    came = holds[parts - recent:]
    at = features + LANES
    blocks = (own_ref.shape[1] - at) // width
    bad = None
    known = []
    for i, ref in enumerate((own_ref, *came)):
        flag = jnp.max(ref[:, features:features + LANES].astype(f32)[:, 4:5], axis=0, keepdims=True)
        bad = flag if bad is None else jnp.maximum(bad, flag)
        for j in range(blocks):
            value = ref[:, at + j * width:at + (j + 1) * width].astype(f32)
            if count >= room:
                known.append(value)
                continue
            rows = ref.shape[0]
            to = lax.broadcasted_iota(jnp.int32, (room, rows), 0)
            source = lax.broadcasted_iota(jnp.int32, (room, rows), 1)
            shift = (i * count) % room
            put = jnp.where((to == source + shift) & (source < count), 1.0, 0.0)
            value = jnp.dot(put, value, preferred_element_type=f32)
            if (i * count) // room == len(known):
                known.append(value)
            else:
                known[-1] = known[-1] + value
    bad = jnp.maximum(bad, crowding(known, owners, fields, near_axes, axis, room, spot_ref))
    moved = select(holds, near_axes, axis, room, spot_ref, (features,))
    finish(moved, known, bad, room, features, send_refs)


def final_body(cap, slots, owners, fields, width, features, groups, parts, spot_ref, id_col_ref, id_row_ref, tokens_ref, *refs):
    f32, i32 = jnp.float32, jnp.int32
    known_refs, holds = refs[:parts[0]], refs[parts[0]:parts[0] + parts[1]]
    out_ref, adv_ref, flag_ref, wide, out, extra, more, slot_v, weight_v, slot_s, weight_s, table_sems, out_sems = refs[parts[0] + parts[1]:]
    total, pieces = out.shape[0], out_sems.shape[0]
    main = tokens_ref.shape[0]
    half = features // LANES
    bad = jnp.zeros((1, LANES), f32)
    for ref in known_refs:
        bad = jnp.maximum(bad, jnp.max(ref[:, features:features + LANES].astype(f32), axis=0, keepdims=True))
    bad = jnp.where(lax.broadcasted_iota(i32, (1, LANES), 1) == 4, bad, 0.0)
    flag_ref[0] = jnp.max(bad).astype(i32)
    lane = lax.broadcasted_iota(i32, (width, LANES), 0)
    column = lax.broadcasted_iota(i32, (width, LANES), 1)
    mine = jnp.where(((lane >> (owners.bit_length() - 1)) == column) & ((lane & (owners - 1)) == spot_ref[0]) & (lane < fields - owners), 1.0, 0.0)
    entry = []
    for ref in known_refs:
        for j in range((ref.shape[1] - features - LANES) // width):
            at = features + LANES + j * width
            entry.append(jnp.dot(ref[:, at:at + width].astype(f32), mine, preferred_element_type=f32))
    entry = jnp.concatenate(entry, axis=0)
    turned = entry.T
    ids, ids_row = id_col_ref[...], id_row_ref[...]
    label = [entry[:, k:k + 1] for k in range(slots)]
    size = [entry[:, slots + k:slots + k + 1] for k in range(slots)]
    level = [entry[:, 2 * slots + k:2 * slots + k + 1] for k in range(slots)]
    if holds:
        info = jnp.concatenate([ref[:, features:features + LANES].astype(f32) for ref in holds], axis=0)
        there = info.T
        key = jnp.where((there[0:1] > 0) & (there[1:2] == spot_ref[0].astype(f32)), there[2:3] * 256.0 + there[3:4], -1.0)
        held_at = lax.broadcasted_iota(i32, (owners, key.shape[1]), 1).astype(f32)
    q = lax.broadcasted_iota(i32, (owners, total), 1).astype(f32)
    rows = [jnp.zeros((1, total), f32) for _ in range(4)]
    pos = jnp.zeros((owners, 1), f32)
    for k in range(slots):
        rank = jnp.zeros((owners, owners), f32)
        for j in range(slots):
            ahead = (ids_row < ids) if j >= k else (ids_row <= ids)
            rank = rank + jnp.where((label[k] == turned[j:j + 1, :]) & ahead, 1.0, 0.0)
        target = jnp.where(label[k] > 0, (label[k] - 1.0) * G + jnp.sum(rank, axis=1, keepdims=True), -1.0)
        places = []
        for t in range(2):
            p = pos if t == 0 else pos + jnp.where(size[k] > 1, 1.0, 0.0)
            place = ids * cap + p
            if holds:
                hit = jnp.where(key == ids * 256.0 + p, held_at, 0.0)
                place = jnp.where(p < cap, place, main + jnp.sum(hit, axis=1, keepdims=True))
            places.append(place)
        hit = target == q
        for r, v in enumerate((*places, size[k], level[k])):
            rows[r] = rows[r] + jnp.sum(jnp.where(hit, v, 0.0), axis=0, keepdims=True)
        pos = pos + size[k]
    slot_v[0:1, :] = rows[0].astype(i32)
    slot_v[1:2, :] = rows[1].astype(i32)
    n, lv = rows[2], rows[3]
    a = lax.broadcasted_iota(i32, (total, total), 0) // G
    b = lax.broadcasted_iota(i32, (total, total), 1) // G
    group = jnp.where(a == b, 1.0, 0.0)
    mean = jnp.dot(lv, group, preferred_element_type=f32) * (1.0 / G)
    square = jnp.dot(lv * lv, group, preferred_element_type=f32) * (1.0 / G)
    spread = jnp.sqrt(square - mean * mean)
    advantage = (lv - mean) / jnp.maximum(spread, 1.0)
    adv_ref[...] = advantage
    weight_v[0:1, :] = advantage / n
    weight_v[1:2, :] = jnp.where(n > 1, advantage / n, 0.0)
    copy_slot = pltpu.make_async_copy(slot_v, slot_s, table_sems.at[0])
    copy_weight = pltpu.make_async_copy(weight_v, weight_s, table_sems.at[1])
    copy_slot.start()
    copy_weight.start()
    base = 0
    for ref in holds:
        p = ref.shape[0]
        for c in range(half):
            extra[base:base + p, c, :] = ref[:, c * LANES:(c + 1) * LANES].astype(f32)
        base += p
    for h in range(base):
        more[h] = extra[h].astype(jnp.bfloat16)
    copy_slot.wait()
    copy_weight.wait()

    batch = wide.shape[0]
    piece = total // pieces

    def work(j, _):
        for e in range(batch):
            i = j * batch + e
            for t in range(2):
                at = slot_s[t, i]
                x = tokens_ref[jnp.minimum(at, main - 1)]
                if holds:
                    x = jnp.where(at < main, x, more[jnp.maximum(at - main, 0)])
                x = x.astype(f32)
                wide[e, pl.ds(t, half, stride=2), :] = x * weight_s[t, i]
        for e in range(batch):
            out[j * batch + e] = wide[e].astype(jnp.bfloat16)
        return 0

    def chunk(k, _):
        lax.fori_loop(k * (piece // batch), (k + 1) * (piece // batch), work, 0)
        part = pl.ds(k * piece, piece)
        pltpu.make_async_copy(out.at[part], out_ref.at[part], out_sems.at[k]).start()
        return 0
    lax.fori_loop(0, pieces, chunk, 0)
    for k in range(pieces):
        part = pl.ds(k * piece, piece)
        pltpu.make_async_copy(out.at[part], out_ref.at[part], out_sems.at[k]).wait()


SMEM = pl.BlockSpec(memory_space=pltpu.SMEM)
VMEM = pl.BlockSpec(memory_space=pltpu.VMEM)
HBM = pl.BlockSpec(memory_space=pltpu.HBM)
ROOM = pltpu.CompilerParams(vmem_limit_bytes=20 << 20)
COST = pl.CostEstimate(flops=1 << 20, bytes_accessed=1 << 20, transcendentals=0)


def pack(spot, rows, gain, prompt_of, lengths, owners, cap, groups, limit):
    total, width, _ = rows.shape
    half = width // 2
    few = max(limit, 16)
    return pl.pallas_call(
        functools.partial(pack_body, cap, groups, limit),
        out_shape=[
            jax.ShapeDtypeStruct((owners * cap, half, LANES), jnp.bfloat16),
            jax.ShapeDtypeStruct((few, half, LANES), jnp.bfloat16),
            jax.ShapeDtypeStruct((few, LANES), jnp.bfloat16),
            jax.ShapeDtypeStruct((1, total), jnp.int32),
        ],
        in_specs=[SMEM, VMEM, VMEM, VMEM, HBM],
        out_specs=[VMEM, VMEM, VMEM, VMEM],
        scratch_shapes=[
            pltpu.VMEM(rows.shape, jnp.bfloat16),
            pltpu.VMEM((BATCH, width, LANES), jnp.float32),
            pltpu.VMEM((2 * total, half, LANES), jnp.bfloat16),
            pltpu.VMEM((2, total), jnp.int32),
            pltpu.VMEM((few, LANES), jnp.int32),
            pltpu.SMEM((2, total), jnp.int32),
            pltpu.SMEM((few, LANES), jnp.int32),
            pltpu.SemaphoreType.DMA((8,)),
            pltpu.SemaphoreType.DMA((2,)),
        ],
        cost_estimate=COST, compiler_params=ROOM,
        name="pack",
    )(spot, prompt_of, lengths, gain, rows)


def log2(n):
    assert n & (n - 1) == 0
    return n.bit_length() - 1


def on_device(hidden, norm_gain, prompt_of, lengths, reward_level):
    f32, i32, bf16 = jnp.float32, jnp.int32, jnp.bfloat16
    count_here, window, features = hidden.shape
    sizes = {a: lax.axis_size(a) for a in AXES}
    owners = sizes["gx"] * sizes["gy"] * sizes["gz"]
    slots = max(2, count_here // owners + 1)
    mean = window * count_here // owners
    full = window * slots
    cap = min(full, max(window, mean - mean // 8))
    limit, room = 16, 8
    groups = count_here // G
    half = features // LANES
    stride = {"gx": sizes["gy"] * sizes["gz"], "gy": sizes["gz"], "gz": 1}
    coord = {a: lax.axis_index(a) for a in AXES}
    me = sum(coord[a] * stride[a] for a in AXES)
    stages = [("gz", 0, sizes["gz"]), ("gx", 0, sizes["gx"])]
    stages += [("gy", bit, 2) for bit in range(log2(sizes["gy"]))]
    spot = jnp.stack([me] + [(coord[a] >> bit) & (n - 1) for a, bit, n in stages]).astype(i32)
    fields = 3 * slots * owners + owners
    width = -(-fields // LANES) * LANES

    rows = hidden.reshape(count_here, window, half, LANES).transpose(0, 2, 1, 3)
    rows = rows.reshape(count_here, window * half, LANES)
    gain = norm_gain.reshape(half, LANES)
    prompts, sizes_of, levels = prompt_of[None], lengths[None], reward_level[None]
    sent, spill, marks, nth = pack(spot, rows, gain, prompts, sizes_of, owners, cap, groups, limit)
    came = lax.all_to_all(sent, AXES, split_axis=0, concat_axis=0, tiled=True)

    lanes = features + LANES
    shape = functools.partial(jax.ShapeDtypeStruct, dtype=bf16)
    holds, got, own, near, count, before = [], [], None, [], 1, 0
    steps = {a: np.zeros((1,), np.int32) for a in AXES}
    for n, (a, bit, size) in enumerate(stages):
        axis = (size, log2(stride[a]) + bit, n + 1)
        with jax.named_scope("stage" + str(n)):
            if n == 0:
                hold, *sends = pl.pallas_call(
                    functools.partial(first_body, tuple(near), axis, room, owners, fields, width, cap, groups),
                    out_shape=[shape((limit, lanes + width))] + [shape((room, lanes + width))] * (size - 1),
                    in_specs=[SMEM] + [VMEM] * 6, out_specs=[VMEM] * size,
                    scratch_shapes=[pltpu.VMEM((limit, half, LANES), f32)],
                    cost_estimate=COST, compiler_params=ROOM, name="stage",
                )(spot, prompts, sizes_of, levels, nth, marks, spill)
                holds = [hold]
            else:
                blocks = -(-count // room)
                sends = pl.pallas_call(
                    functools.partial(next_body, tuple(near), axis, room, owners, fields, width, before, features, len(holds), len(got)),
                    out_shape=[shape((room, lanes + blocks * width))] * (size - 1),
                    in_specs=[SMEM] + [VMEM] * (len(holds) + 1), out_specs=[VMEM] * (size - 1),
                    cost_estimate=COST, compiler_params=ROOM, name="stage",
                )(spot, *holds, own)
            got = []
            for k in range(1, size):
                pairs = [(i, i ^ (k << bit)) for i in range(sizes[a])]
                got.append(lax.ppermute(sends[k - 1], a, pairs))
            own = sends[0]
            holds = holds + got
        near.append(axis)
        before = count
        count *= size
        steps = {x: np.concatenate([v + ((k << bit) if x == a else 0) for k in range(size)]).astype(np.int32) for x, v in steps.items()}

    ids = sum((coord[a] ^ steps[a]) * stride[a] for a in AXES).astype(f32)
    known = [own, *got]

    def finish_with(tokens, cap_used, extras):
        spare = sum(h.shape[0] for h in extras)
        return pl.pallas_call(
            functools.partial(final_body, cap_used, slots, owners, fields, width, features, groups, (len(known), len(extras))),
            out_shape=[
                jax.ShapeDtypeStruct((count_here, window * half, LANES), bf16),
                jax.ShapeDtypeStruct((1, count_here), f32),
                jax.ShapeDtypeStruct((1,), i32),
            ],
            in_specs=[SMEM] + [VMEM] * (3 + len(known) + len(extras)), out_specs=[HBM, VMEM, SMEM],
            scratch_shapes=[
                pltpu.VMEM((BATCH, window * half, LANES), f32),
                pltpu.VMEM((count_here, window * half, LANES), bf16),
                pltpu.VMEM((max(spare, 8), half, LANES), f32),
                pltpu.VMEM((max(spare, 8), half, LANES), bf16),
                pltpu.VMEM((window, count_here), i32),
                pltpu.VMEM((window, count_here), f32),
                pltpu.SMEM((window, count_here), i32),
                pltpu.SMEM((window, count_here), f32),
                pltpu.SemaphoreType.DMA((2,)),
                pltpu.SemaphoreType.DMA((8,)),
            ],
            cost_estimate=COST, compiler_params=ROOM, name="place",
        )(spot, ids[:, None], ids[None], tokens, *known, *extras)

    def whole(out):
        out = out.reshape(count_here, half, window, LANES).transpose(0, 2, 1, 3)
        return out.reshape(count_here, window, features)
    out, advantages, bad = finish_with(came, cap, holds)

    def crowded(state):
        again = pack(spot, rows, gain, prompts, sizes_of, owners, full, groups, 0)
        all_came = lax.all_to_all(again[0], AXES, split_axis=0, concat_axis=0, tiled=True)
        return jnp.zeros((1,), i32), whole(finish_with(all_came, full, [])[0])
    _, out = lax.while_loop(lambda state: state[0][0] > 0, crowded, (bad, whole(out)))
    return out, advantages.reshape(count_here)


def solution(mesh):
    many = P(AXES)
    return jax.shard_map(
        on_device, mesh=mesh,
        in_specs=(P(AXES, None, None), P(), many, many, many),
        out_specs=(P(AXES, None, None), many), check_vma=False,
    )
```

```python
import functools
import jax
import numpy as np
import jax.numpy as jnp
from jax import lax
from jax.experimental import pallas as pl
from jax.experimental.pallas import tpu as pltpu
from jax.sharding import PartitionSpec as P

G = 16
AXES = ("gx", "gy", "gz")
LANES = 128
BATCH = 16
norm_eps = 1e-05


def pack_body(cap, groups, limit, spot_ref, prompt_ref, length_ref, gain_ref, rows_ref,
              out_ref, spill_ref, mark_ref, nth_ref,
              rows, wide, tokens, way_v, list_v, way, spilled, in_sems, way_sems):
    f32, i32 = jnp.float32, jnp.int32
    total, pieces = rows.shape[0], in_sems.shape[0]
    piece = total // pieces
    batch = wide.shape[0]
    half = wide.shape[1] // 2
    features = half * LANES
    for k in range(pieces):
        part = pl.ds(k * piece, piece)
        pltpu.make_async_copy(rows_ref.at[part], rows.at[part], in_sems.at[k]).start()

    p, n = prompt_ref[...], length_ref[...]
    column = jnp.broadcast_to((p * 4 + n).astype(f32), (total, total)).T.astype(i32)
    before = lax.broadcasted_iota(i32, (total, total), 0) < lax.broadcasted_iota(i32, (total, total), 1)
    owner = p >> log2(groups)
    same = ((column >> (2 + log2(groups))) == owner) & before
    at = jnp.sum(jnp.where(same, column & 3, 0), axis=0, keepdims=True)
    nth_ref[...] = jnp.sum(jnp.where(same, 1, 0), axis=0, keepdims=True)
    lane = lax.broadcasted_iota(i32, (1, total), 1)
    home = jnp.sum(jnp.where(lane == 0, owner, 0), axis=1, keepdims=True) * cap
    d0 = jnp.where(at < cap, owner * cap + at, home)
    way_v[0:1, :] = d0
    way_v[1:2, :] = jnp.where((n > 1) & (at + 1 < cap), d0 + 1, d0)
    pltpu.make_async_copy(way_v, way, way_sems.at[0]).start()
    if limit:
        over = jnp.where(at >= cap, 1, 0)
        more = jnp.where((n > 1) & (at + 1 >= cap), 1, 0)
        start = jnp.dot((over + more).astype(f32), jnp.where(before, 1.0, 0.0), preferred_element_type=f32).astype(i32)
        e = lax.broadcasted_iota(i32, (limit, total), 0)
        hit0 = (over > 0) & (start == e)
        hit1 = (more > 0) & (start + over == e)
        token = jnp.sum(jnp.where(hit0, 2 * lane + 1, jnp.where(hit1, 2 * lane + 2, 0)), axis=1, keepdims=True)
        dest = jnp.sum(jnp.where(hit0 | hit1, owner, 0), axis=1, keepdims=True)
        spot = jnp.sum(jnp.where(hit0, at, jnp.where(hit1, at + 1, 0)), axis=1, keepdims=True)
        lanes = lax.broadcasted_iota(i32, (limit, LANES), 1)
        mark = jnp.where(lanes == 0, 1, jnp.where(lanes == 1, dest, jnp.where(lanes == 2, spot_ref[0], jnp.where(lanes == 3, spot, 0))))
        mark_ref[...] = jnp.where(token > 0, mark, 0).astype(f32).astype(jnp.bfloat16)
        list_v[...] = jnp.broadcast_to(jnp.maximum(token - 1, 0), list_v.shape)
        pltpu.make_async_copy(list_v, spilled, way_sems.at[1]).start()
    else:
        mark_ref[...] = jnp.zeros(mark_ref.shape, mark_ref.dtype)
    gain = gain_ref[...]
    pltpu.make_async_copy(way_v, way, way_sems.at[0]).wait()

    def work(j, _):
        for b in range(batch):
            wide[b] = rows[j * batch + b].astype(f32)
        for b in range(batch):
            i = j * batch + b
            for t in (1, 0):
                x = wide[b, pl.ds(t, half, stride=2), :]
                s = jnp.sum((x * x).reshape(half // 8, 8, LANES), axis=0)
                s = jnp.sum(jnp.sum(s, axis=1, keepdims=True), axis=0, keepdims=True)
                r = lax.rsqrt(s * (1.0 / features) + norm_eps)
                x = (x * r * gain).astype(jnp.bfloat16)
                out_ref[way[t, i]] = x
                tokens[2 * i + t] = x
        return 0

    per = piece // batch

    def chunk(k, _):
        part = pl.ds(k * piece, piece)
        pltpu.make_async_copy(rows_ref.at[part], rows.at[part], in_sems.at[k]).wait()
        return lax.fori_loop(k * per, (k + 1) * per, work, 0)

    lax.fori_loop(0, pieces, chunk, 0)
    out_ref[way[0, 0]] = tokens[0]
    if limit:
        pltpu.make_async_copy(list_v, spilled, way_sems.at[1]).wait()
        for e in range(limit):
            spill_ref[e] = tokens[spilled[e, 0]]
    else:
        spill_ref[...] = jnp.zeros(spill_ref.shape, spill_ref.dtype)


def select(parts, near_axes, axis, room, spot_ref, shape):
    f32 = jnp.float32
    size, stride, mine = axis
    moved, offset = None, jnp.zeros((1, LANES), f32)
    for ref in parts:
        p = ref.shape[0]
        info = ref[:, shape[0]:shape[0] + LANES].astype(f32)
        dest = info[:, 1:2].astype(jnp.int32)
        lane = lax.broadcasted_iota(jnp.int32, (p, LANES), 1)
        go = (lane < (size - 1) * room) & (info[:, 0:1] > 0)
        for n, st, at in near_axes:
            go = go & (((dest >> st) & (n - 1)) == spot_ref[at])
        turn = lane & (room - 1)
        to = spot_ref[mine] ^ ((lane >> (room.bit_length() - 1)) + 1)
        go = jnp.where(go & (((dest >> stride) & (size - 1)) == to), 1.0, 0.0)
        row = lax.broadcasted_iota(jnp.int32, (p, p), 0)
        col = lax.broadcasted_iota(jnp.int32, (p, p), 1)
        nth = jnp.dot(jnp.where(col < row, 1.0, 0.0), go, preferred_element_type=f32) + offset
        offset = offset + jnp.sum(go, axis=0, keepdims=True)
        pick = jnp.where(nth == turn.astype(f32), go, 0.0)[:, :(size - 1) * room]
        data = ref[:, :shape[0] + LANES].astype(f32)
        part = lax.dot_general(pick, data, (((0,), (0,)), ((), ())), preferred_element_type=f32)
        moved = part if moved is None else moved + part
    return moved


def crowding(known, owners, fields, near_axes, axis, room, spot_ref):
    f32 = jnp.float32
    size, stride, mine = axis
    o = lax.broadcasted_iota(jnp.int32, (owners, LANES), 0)
    b = lax.broadcasted_iota(jnp.int32, (owners, LANES), 1)
    at = (o >> stride) & (size - 1)
    place = at
    span = size
    for n, st, _ in near_axes:
        place = place + span * ((o >> st) & (n - 1))
        span *= n
    member = jnp.where((place == b) & (at != spot_ref[mine]), 1.0, 0.0)
    total = jnp.zeros((1, LANES), f32)
    for k in known:
        left = jnp.sum(k[:, fields - owners:fields], axis=0, keepdims=True)
        total = total + jnp.dot(left, member, preferred_element_type=f32)
    return jnp.max(jnp.where(total > room, 1.0, 0.0), axis=1, keepdims=True)


def first_body(near_axes, axis, room, owners, fields, width, cap, groups, spot_ref, prompt_ref, length_ref, level_ref, nth_ref, mark_ref, spill_ref, hold_ref, *rest):
    f32, i32 = jnp.float32, jnp.int32
    limit, half, _ = spill_ref.shape
    features = half * LANES
    send_refs, wide = rest[:-1], rest[-1]
    wide[...] = spill_ref[...].astype(f32)
    for c in range(half):
        hold_ref[:, c * LANES:(c + 1) * LANES] = wide[:, c, :].astype(jnp.bfloat16)
    hold_ref[:, features:features + LANES] = mark_ref[...]
    p, n = prompt_ref[...], length_ref[...]
    total = p.shape[1]
    owner = p >> log2(groups)
    place = nth_ref[...] * owners + owner
    column = jnp.broadcast_to(place.astype(f32), (total, total)).T.astype(i32)[:, :1]
    lane = lax.broadcasted_iota(i32, (total, width), 1)
    block = (fields - owners) // 3
    own = jnp.zeros((1, width), f32)
    for k, v in enumerate(((p & (groups - 1)) + 1, n, level_ref[...])):
        here = jnp.where(lane == column + k * block, 1.0, 0.0)
        own = own + jnp.dot(v.astype(f32), here, preferred_element_type=f32)
    here = jnp.where(lane == (column & (owners - 1)) + 3 * block, 1.0, 0.0)
    tokens = jnp.dot(n.astype(f32), here, preferred_element_type=f32)
    own = own + jnp.maximum(tokens - cap, 0.0)
    first = lax.broadcasted_iota(i32, (limit, width), 0) == 0
    known = jnp.where(first, own, 0.0)
    hold_ref[:, features + LANES:] = known.astype(jnp.bfloat16)
    left = jnp.sum(own[:, fields - owners:fields], axis=1, keepdims=True)
    bad = jnp.where(left > limit, 1.0, 0.0)
    bad = jnp.maximum(bad, crowding([known], owners, fields, near_axes, axis, room, spot_ref))
    moved = select([hold_ref], near_axes, axis, room, spot_ref, (features,))
    finish(moved, [known[:room]], bad, room, features, send_refs)


def finish(moved, known, bad, room, features, send_refs):
    rows = moved.shape[0]
    lane = lax.broadcasted_iota(jnp.int32, (rows, LANES), 1)
    info = jnp.where(lane == 4, bad, jnp.where(lane < 4, moved[:, features:], 0.0))
    for k, send_ref in enumerate(send_refs):
        part = slice(k * room, (k + 1) * room)
        send_ref[:, :features] = moved[part, :features].astype(jnp.bfloat16)
        send_ref[:, features:features + LANES] = info[part].astype(jnp.bfloat16)
        at = features + LANES
        for v in known:
            send_ref[:, at:at + v.shape[1]] = v.astype(jnp.bfloat16)
            at += v.shape[1]


def next_body(near_axes, axis, room, owners, fields, width, count, features, parts, recent, last, spot_ref, *refs):
    f32 = jnp.float32
    holds, own_ref, send_refs = refs[:parts], refs[parts], refs[parts + 1:]
    came = holds[parts - recent:]
    at = features + LANES
    blocks = (own_ref.shape[1] - at) // width
    bad = None
    known = []
    for i, ref in enumerate((own_ref, *came)):
        flag = jnp.max(ref[:, features:features + LANES].astype(f32)[:, 4:5], axis=0, keepdims=True)
        bad = flag if bad is None else jnp.maximum(bad, flag)
        for j in range(blocks):
            value = ref[:, at + j * width:at + (j + 1) * width].astype(f32)
            if count >= room:
                known.append(value)
                continue
            rows = ref.shape[0]
            to = lax.broadcasted_iota(jnp.int32, (room, rows), 0)
            source = lax.broadcasted_iota(jnp.int32, (room, rows), 1)
            shift = (i * count) % room
            put = jnp.where((to == source + shift) & (source < count), 1.0, 0.0)
            value = jnp.dot(put, value, preferred_element_type=f32)
            if (i * count) // room == len(known):
                known.append(value)
            else:
                known[-1] = known[-1] + value
    bad = jnp.maximum(bad, crowding(known, owners, fields, near_axes, axis, room, spot_ref))
    moved = select(holds, near_axes, axis, room, spot_ref, (features,))
    if not last:
        finish(moved, known, bad, room, features, send_refs)
        return
    token_ref, entry_ref, own_entry_ref = send_refs
    rows = len(known) * room
    for ref, who in ((own_entry_ref, spot_ref[0]), (entry_ref, spot_ref[0] ^ (1 << axis[1]))):
        lane = lax.broadcasted_iota(jnp.int32, (width, LANES), 0)
        column = lax.broadcasted_iota(jnp.int32, (width, LANES), 1)
        mine = jnp.where(((lane >> log2(owners)) == column) & ((lane & (owners - 1)) == who) & (lane < fields - owners), 1.0, 0.0)
        for j, v in enumerate(known):
            ref[j * room:(j + 1) * room, :] = jnp.dot(v, mine, preferred_element_type=f32).astype(jnp.bfloat16)
        lane = lax.broadcasted_iota(jnp.int32, (room, LANES), 1)
        info = jnp.where(lane == 4, bad, jnp.where(lane < 4, moved[:, features:], 0.0))
        ref[rows:rows + room, :] = info.astype(jnp.bfloat16)
    token_ref[...] = moved[:, :features].astype(jnp.bfloat16)


def plan_body(cap, full, slots, owners, features, main, room, batch, spot_ref, id_col_ref, id_row_ref, own_ref, got_ref, *refs):
    f32, i32 = jnp.float32, jnp.int32
    holds, (slot_ref, weight_ref, adv_ref, flag_ref) = refs[:-4], refs[-4:]
    rows = owners // 2
    total = slot_ref.shape[1]
    info = [ref[:, features:features + LANES].astype(f32) for ref in holds] + [got_ref[rows:rows + room, :].astype(f32)]
    bad = jnp.max(jnp.maximum(info[-1], own_ref[rows:rows + room, :].astype(f32)), axis=0, keepdims=True)
    bad = jnp.where(lax.broadcasted_iota(i32, (1, LANES), 1) == 4, bad, 0.0)
    flag_ref[0] = jnp.max(bad).astype(i32)
    there = jnp.concatenate(info, axis=0).T
    entry = jnp.concatenate([own_ref[:rows, :].astype(f32), got_ref[:rows, :].astype(f32)], axis=0)
    turned = entry.T
    ids, ids_row = id_col_ref[...], id_row_ref[...]
    label = [entry[:, k:k + 1] for k in range(slots)]
    size = [entry[:, slots + k:slots + k + 1] for k in range(slots)]
    level = [entry[:, 2 * slots + k:2 * slots + k + 1] for k in range(slots)]
    key = jnp.where((there[0:1] > 0) & (there[1:2] == spot_ref[0].astype(f32)), there[2:3] * 256.0 + there[3:4], -1.0)
    held_at = lax.broadcasted_iota(i32, (owners, key.shape[1]), 1).astype(f32)
    q = lax.broadcasted_iota(i32, (owners, total), 1).astype(f32)
    found = [jnp.zeros((owners, total), f32) for _ in range(5)]
    pos = jnp.zeros((owners, 1), f32)
    for k in range(slots):
        rank = jnp.zeros((owners, owners), f32)
        for j in range(slots):
            ahead = (ids_row < ids) if j >= k else (ids_row <= ids)
            rank = rank + jnp.where((label[k] == turned[j:j + 1, :]) & ahead, 1.0, 0.0)
        target = jnp.where(label[k] > 0, (label[k] - 1.0) * G + jnp.sum(rank, axis=1, keepdims=True), -1.0)
        places = []
        for t in range(2):
            p = pos if t == 0 else pos + jnp.where(size[k] > 1, 1.0, 0.0)
            place = ids * cap + p
            if 2 * k + t >= cap:
                held = jnp.sum(jnp.where(key == ids * 256.0 + p, held_at, 0.0), axis=1, keepdims=True)
                place = jnp.where(p < cap, place, main + held)
            places.append(place)
        hit = target == q
        for r, v in enumerate((*places, size[k], level[k], ids * full + pos)):
            found[r] = jnp.where(hit, v, found[r])
        pos = pos + size[k]
    one, two, n, lv, far = (jnp.sum(v, axis=0, keepdims=True) for v in found)
    a = lax.broadcasted_iota(i32, (total, total), 0)
    b = lax.broadcasted_iota(i32, (total, total), 1)
    spare = jnp.where(jnp.maximum(one, two) >= main, 1.0, 0.0)
    near = jnp.where(a >> log2(batch) == b >> log2(batch), 1.0, 0.0)
    slot_ref[0:1, :] = one.astype(i32)
    slot_ref[1:2, :] = two.astype(i32)
    slot_ref[2:3, :] = jnp.dot(spare, near, preferred_element_type=f32).astype(i32)
    slot_ref[3:4, :] = far.astype(i32)
    slot_ref[4:5, :] = (far + jnp.where(n > 1, 1.0, 0.0)).astype(i32)
    slot_ref[5:8, :] = jnp.zeros((3, total), i32)
    group = jnp.where(a >> log2(G) == b >> log2(G), 1.0, 0.0)
    mean = jnp.dot(lv, group, preferred_element_type=f32) * (1.0 / G)
    square = jnp.dot(lv * lv, group, preferred_element_type=f32) * (1.0 / G)
    spread = jnp.sqrt(square - mean * mean)
    advantage = (lv - mean) / jnp.maximum(spread, 1.0)
    adv_ref[...] = advantage
    weight_ref[0:1, :] = advantage / n
    weight_ref[1:2, :] = jnp.where(n > 1, advantage / n, 0.0)


def place_body(row, slot_ref, weight_ref, tokens_ref, *refs):
    f32 = jnp.float32
    holds, (out_ref, wide, out, extra, more, slot_s, weight_s, table_sems, out_sems) = refs[:-9], refs[-9:]
    copy_slot = pltpu.make_async_copy(slot_ref, slot_s, table_sems.at[0])
    copy_weight = pltpu.make_async_copy(weight_ref, weight_s, table_sems.at[1])
    copy_slot.start()
    copy_weight.start()
    pieces = out_sems.shape[0]
    main = tokens_ref.shape[0]
    batch, half = wide.shape[0], wide.shape[1] // 2
    base = 0
    for ref in holds:
        p = ref.shape[0]
        for c in range(half):
            extra[base:base + p, c, :] = ref[:, c * LANES:(c + 1) * LANES].astype(f32)
        base += p
    for h in range(base):
        more[h] = extra[h].astype(jnp.bfloat16)
    copy_slot.wait()
    copy_weight.wait()

    def work(j, mixed):
        for e in range(batch):
            i = j * batch + e
            for t in range(2):
                at = slot_s[row + t, i]
                if mixed:
                    x = tokens_ref[jnp.minimum(at, main - 1)]
                    x = jnp.where(at < main, x, more[jnp.maximum(at - main, 0)])
                else:
                    x = tokens_ref[at]
                wide[e, pl.ds(t, half, stride=2), :] = x.astype(f32) * weight_s[t, i]
        for e in range(batch):
            out[j * batch + e] = wide[e].astype(jnp.bfloat16)

    def chunk(k, _):
        if holds:
            @pl.when(slot_s[2, k * batch] == 0)
            def _():
                work(k, False)

            @pl.when(slot_s[2, k * batch] > 0)
            def _():
                work(k, True)
        else:
            work(k, False)
        part = pl.ds(k * batch, batch)
        pltpu.make_async_copy(out.at[part], out_ref.at[part], out_sems.at[k]).start()
        return 0

    lax.fori_loop(0, pieces, chunk, 0)
    for k in range(pieces):
        part = pl.ds(k * batch, batch)
        pltpu.make_async_copy(out.at[part], out_ref.at[part], out_sems.at[k]).wait()


SMEM = pl.BlockSpec(memory_space=pltpu.SMEM)
VMEM = pl.BlockSpec(memory_space=pltpu.VMEM)
HBM = pl.BlockSpec(memory_space=pltpu.HBM)
ROOM = pltpu.CompilerParams(vmem_limit_bytes=20 << 20)
COST = pl.CostEstimate(flops=1 << 20, bytes_accessed=1 << 20, transcendentals=0)


def pack(spot, rows, gain, prompt_of, lengths, owners, cap, groups, limit):
    total, width, _ = rows.shape
    half = width // 2
    few = max(limit, 16)
    return pl.pallas_call(
        functools.partial(pack_body, cap, groups, limit),
        out_shape=[
            jax.ShapeDtypeStruct((owners * cap, half, LANES), jnp.bfloat16),
            jax.ShapeDtypeStruct((few, half, LANES), jnp.bfloat16),
            jax.ShapeDtypeStruct((few, LANES), jnp.bfloat16),
            jax.ShapeDtypeStruct((1, total), jnp.int32),
        ],
        in_specs=[SMEM, VMEM, VMEM, VMEM, HBM],
        out_specs=[VMEM, VMEM, VMEM, VMEM],
        scratch_shapes=[
            pltpu.VMEM(rows.shape, jnp.bfloat16),
            pltpu.VMEM((BATCH, width, LANES), jnp.float32),
            pltpu.VMEM((2 * total, half, LANES), jnp.bfloat16),
            pltpu.VMEM((2, total), jnp.int32),
            pltpu.VMEM((few, LANES), jnp.int32),
            pltpu.SMEM((2, total), jnp.int32),
            pltpu.SMEM((few, LANES), jnp.int32),
            pltpu.SemaphoreType.DMA((8,)),
            pltpu.SemaphoreType.DMA((2,)),
        ],
        cost_estimate=COST, compiler_params=ROOM,
        name="pack",
    )(spot, prompt_of, lengths, gain, rows)


def log2(n):
    assert n & (n - 1) == 0
    return n.bit_length() - 1


def on_device(hidden, norm_gain, prompt_of, lengths, reward_level):
    f32, i32, bf16 = jnp.float32, jnp.int32, jnp.bfloat16
    count_here, window, features = hidden.shape
    sizes = {a: lax.axis_size(a) for a in AXES}
    owners = sizes["gx"] * sizes["gy"] * sizes["gz"]
    slots = max(2, count_here // owners + 1)
    mean = window * count_here // owners
    full = window * slots
    cap = min(full, max(window, mean - mean // 8))
    limit, room = 16, 8
    groups = count_here // G
    half = features // LANES
    stride = {"gx": sizes["gy"] * sizes["gz"], "gy": sizes["gz"], "gz": 1}
    coord = {a: lax.axis_index(a) for a in AXES}
    me = sum(coord[a] * stride[a] for a in AXES)
    stages = [("gz", 0, sizes["gz"]), ("gx", 0, sizes["gx"])]
    stages += [("gy", bit, 2) for bit in range(log2(sizes["gy"]))]
    spot = jnp.stack([me] + [(coord[a] >> bit) & (n - 1) for a, bit, n in stages]).astype(i32)
    fields = 3 * slots * owners + owners
    width = -(-fields // LANES) * LANES

    rows = hidden.reshape(count_here, window, half, LANES).transpose(0, 2, 1, 3)
    rows = rows.reshape(count_here, window * half, LANES)
    gain = norm_gain.reshape(half, LANES)
    prompts, sizes_of, levels = prompt_of[None], lengths[None], reward_level[None]
    sent, spill, marks, nth = pack(spot, rows, gain, prompts, sizes_of, owners, cap, groups, limit)
    came = lax.all_to_all(sent, AXES, split_axis=0, concat_axis=0, tiled=True)

    lanes = features + LANES
    shape = functools.partial(jax.ShapeDtypeStruct, dtype=bf16)
    holds, got, own, near, count, before = [], [], None, [], 1, 0
    steps = {a: np.zeros((1,), np.int32) for a in AXES}
    for n, (a, bit, size) in enumerate(stages):
        axis = (size, log2(stride[a]) + bit, n + 1)
        if n == 0:
            hold, *sends = pl.pallas_call(
                functools.partial(first_body, tuple(near), axis, room, owners, fields, width, cap, groups),
                out_shape=[shape((limit, lanes + width))] + [shape((room, lanes + width))] * (size - 1),
                in_specs=[SMEM] + [VMEM] * 6, out_specs=[VMEM] * size,
                scratch_shapes=[pltpu.VMEM((limit, half, LANES), f32)],
                cost_estimate=COST, compiler_params=ROOM, name="stage",
            )(spot, prompts, sizes_of, levels, nth, marks, spill)
            holds = [hold]
        else:
            blocks = -(-count // room)
            last = n + 1 == len(stages)
            outs = [shape((room, lanes + blocks * width))] * (size - 1)
            if last:
                outs = [shape((room, features)), shape((count + room, LANES)), shape((count + room, LANES))]
            sends = pl.pallas_call(
                functools.partial(next_body, tuple(near), axis, room, owners, fields, width, before, features, len(holds), len(got), last),
                out_shape=outs,
                in_specs=[SMEM] + [VMEM] * (len(holds) + 1), out_specs=[VMEM] * len(outs),
                cost_estimate=COST, compiler_params=ROOM, name="stage",
            )(spot, *holds, own)
        pairs = [[(i, i ^ (k << bit)) for i in range(sizes[a])] for k in range(size)]
        if n + 1 < len(stages):
            got = [lax.ppermute(sends[k - 1], a, pairs[k]) for k in range(1, size)]
            own = sends[0]
            holds = holds + got
        else:
            own = sends[2]
            entries = lax.ppermute(sends[1], a, pairs[1])
            landed = lax.ppermute(sends[0], a, pairs[1])
        near.append(axis)
        before = count
        count *= size
        steps = {x: np.concatenate([v + ((k << bit) if x == a else 0) for k in range(size)]).astype(np.int32) for x, v in steps.items()}

    ids = sum((coord[a] ^ steps[a]) * stride[a] for a in AXES).astype(f32)
    batch = min(BATCH, count_here)
    vmem_i32 = functools.partial(jax.ShapeDtypeStruct, dtype=i32)
    slot_of, weight, advantages, bad = pl.pallas_call(
        functools.partial(plan_body, cap, full, slots, owners, features, owners * cap, room, batch),
        out_shape=[vmem_i32((8, count_here)), jax.ShapeDtypeStruct((window, count_here), f32), jax.ShapeDtypeStruct((1, count_here), f32), vmem_i32((1,))],
        in_specs=[SMEM] + [VMEM] * (4 + len(holds)), out_specs=[VMEM, VMEM, VMEM, SMEM],
        cost_estimate=COST, compiler_params=ROOM, name="plan",
    )(spot, ids[:, None], ids[None], own, entries, *holds)

    def place(tokens, row, extras):
        spare = max(sum(h.shape[0] for h in extras), 8)
        return pl.pallas_call(
            functools.partial(place_body, row),
            out_shape=jax.ShapeDtypeStruct((count_here, window * half, LANES), bf16),
            in_specs=[VMEM] * (3 + len(extras)), out_specs=HBM,
            scratch_shapes=[
                pltpu.VMEM((batch, window * half, LANES), f32),
                pltpu.VMEM((count_here, window * half, LANES), bf16),
                pltpu.VMEM((spare, half, LANES), f32),
                pltpu.VMEM((spare, half, LANES), bf16),
                pltpu.SMEM((8, count_here), i32),
                pltpu.SMEM((window, count_here), f32),
                pltpu.SemaphoreType.DMA((2,)),
                pltpu.SemaphoreType.DMA((count_here // batch,)),
            ],
            cost_estimate=COST, compiler_params=ROOM, name="place",
        )(slot_of, weight, tokens, *extras)

    def whole(out):
        out = out.reshape(count_here, half, window, LANES).transpose(0, 2, 1, 3)
        return out.reshape(count_here, window, features)

    out = place(came, 0, [*holds, landed])

    def crowded(state):
        again = pack(spot, rows, gain, prompts, sizes_of, owners, full, groups, 0)
        all_came = lax.all_to_all(again[0], AXES, split_axis=0, concat_axis=0, tiled=True)
        return jnp.zeros((1,), i32), whole(place(all_came, 3, []))

    _, out = lax.while_loop(lambda state: state[0][0] > 0, crowded, (bad, whole(out)))
    return out, advantages.reshape(count_here)


def solution(mesh):
    many = P(AXES)
    return jax.shard_map(
        on_device, mesh=mesh,
        in_specs=(P(AXES, None, None), P(), many, many, many),
        out_specs=(P(AXES, None, None), many), check_vma=False,
    )
```

```python
import functools
import jax
import numpy as np
import jax.numpy as jnp
from jax import lax
from jax.experimental import pallas as pl
from jax.experimental.pallas import tpu as pltpu
from jax.sharding import PartitionSpec as P

G = 16
AXES = ("gx", "gy", "gz")
LANES = 128
BATCH = 32
norm_eps = 1e-05


def pack_body(cap, groups, limit, spot_ref, prompt_ref, length_ref, gain_ref, rows_ref,
              out_ref, spill_ref, mark_ref, nth_ref,
              rows, wide, tokens, way_v, list_v, way, spilled, in_sems, way_sems):
    f32, i32 = jnp.float32, jnp.int32
    total, pieces = rows.shape[0], in_sems.shape[0]
    piece = total // pieces
    batch = wide.shape[0]
    half = wide.shape[1] // 2
    features = half * LANES
    for k in range(pieces):
        part = pl.ds(k * piece, piece)
        pltpu.make_async_copy(rows_ref.at[part], rows.at[part], in_sems.at[k]).start()

    p, n = prompt_ref[...], length_ref[...]
    column = jnp.broadcast_to((p * 4 + n).astype(f32), (total, total)).T.astype(i32)
    before = lax.broadcasted_iota(i32, (total, total), 0) < lax.broadcasted_iota(i32, (total, total), 1)
    owner = p >> log2(groups)
    same = ((column >> (2 + log2(groups))) == owner) & before
    at = jnp.sum(jnp.where(same, column & 3, 0), axis=0, keepdims=True)
    nth_ref[...] = jnp.sum(jnp.where(same, 1, 0), axis=0, keepdims=True)
    lane = lax.broadcasted_iota(i32, (1, total), 1)
    home = jnp.sum(jnp.where(lane == 0, owner, 0), axis=1, keepdims=True) * cap
    d0 = jnp.where(at < cap, owner * cap + at, home)
    way_v[0:1, :] = d0
    way_v[1:2, :] = jnp.where((n > 1) & (at + 1 < cap), d0 + 1, d0)
    pltpu.make_async_copy(way_v, way, way_sems.at[0]).start()
    if limit:
        over = jnp.where(at >= cap, 1, 0)
        more = jnp.where((n > 1) & (at + 1 >= cap), 1, 0)
        start = jnp.dot((over + more).astype(f32), jnp.where(before, 1.0, 0.0), preferred_element_type=f32).astype(i32)
        e = lax.broadcasted_iota(i32, (limit, total), 0)
        hit0 = (over > 0) & (start == e)
        hit1 = (more > 0) & (start + over == e)
        token = jnp.sum(jnp.where(hit0, 2 * lane + 1, jnp.where(hit1, 2 * lane + 2, 0)), axis=1, keepdims=True)
        dest = jnp.sum(jnp.where(hit0 | hit1, owner, 0), axis=1, keepdims=True)
        spot = jnp.sum(jnp.where(hit0, at, jnp.where(hit1, at + 1, 0)), axis=1, keepdims=True)
        lanes = lax.broadcasted_iota(i32, (limit, LANES), 1)
        mark = jnp.where(lanes == 0, 1, jnp.where(lanes == 1, dest, jnp.where(lanes == 2, spot_ref[0], jnp.where(lanes == 3, spot, 0))))
        mark_ref[...] = jnp.where(token > 0, mark, 0).astype(f32).astype(jnp.bfloat16)
        list_v[...] = jnp.broadcast_to(jnp.maximum(token - 1, 0), list_v.shape)
        pltpu.make_async_copy(list_v, spilled, way_sems.at[1]).start()
    else:
        mark_ref[...] = jnp.zeros(mark_ref.shape, mark_ref.dtype)
    gain = gain_ref[...]
    pltpu.make_async_copy(way_v, way, way_sems.at[0]).wait()

    def work(j, _):
        for b in range(batch):
            wide[b] = rows[j * batch + b].astype(f32)
        for b in range(batch):
            i = j * batch + b
            for t in (1, 0):
                x = wide[b, pl.ds(t, half, stride=2), :]
                s = jnp.sum((x * x).reshape(half // 8, 8, LANES), axis=0)
                s = jnp.sum(jnp.sum(s, axis=1, keepdims=True), axis=0, keepdims=True)
                r = lax.rsqrt(s * (1.0 / features) + norm_eps)
                x = (x * r * gain).astype(jnp.bfloat16)
                out_ref[way[t, i]] = x
                tokens[2 * i + t] = x
        return 0

    per = piece // batch

    def chunk(k, _):
        part = pl.ds(k * piece, piece)
        pltpu.make_async_copy(rows_ref.at[part], rows.at[part], in_sems.at[k]).wait()
        return lax.fori_loop(k * per, (k + 1) * per, work, 0)

    lax.fori_loop(0, pieces, chunk, 0)
    out_ref[way[0, 0]] = tokens[0]
    if limit:
        pltpu.make_async_copy(list_v, spilled, way_sems.at[1]).wait()
        for e in range(limit):
            spill_ref[e] = tokens[spilled[e, 0]]
    else:
        spill_ref[...] = jnp.zeros(spill_ref.shape, spill_ref.dtype)


def select(parts, near_axes, axis, room, spot_ref, shape):
    f32 = jnp.float32
    size, stride, mine = axis
    moved, offset = None, jnp.zeros((1, LANES), f32)
    for ref in parts:
        p = ref.shape[0]
        info = ref[:, shape[0]:shape[0] + LANES].astype(f32)
        dest = info[:, 1:2].astype(jnp.int32)
        lane = lax.broadcasted_iota(jnp.int32, (p, LANES), 1)
        go = (lane < (size - 1) * room) & (info[:, 0:1] > 0)
        for n, st, at in near_axes:
            go = go & (((dest >> st) & (n - 1)) == spot_ref[at])
        turn = lane & (room - 1)
        to = spot_ref[mine] ^ ((lane >> (room.bit_length() - 1)) + 1)
        go = jnp.where(go & (((dest >> stride) & (size - 1)) == to), 1.0, 0.0)
        row = lax.broadcasted_iota(jnp.int32, (p, p), 0)
        col = lax.broadcasted_iota(jnp.int32, (p, p), 1)
        nth = jnp.dot(jnp.where(col < row, 1.0, 0.0), go, preferred_element_type=f32) + offset
        offset = offset + jnp.sum(go, axis=0, keepdims=True)
        pick = jnp.where(nth == turn.astype(f32), go, 0.0)[:, :(size - 1) * room]
        data = ref[:, :shape[0] + LANES].astype(f32)
        part = lax.dot_general(pick, data, (((0,), (0,)), ((), ())), preferred_element_type=f32)
        moved = part if moved is None else moved + part
    return moved


def crowding(known, owners, fields, near_axes, axis, room, spot_ref):
    f32 = jnp.float32
    size, stride, mine = axis
    o = lax.broadcasted_iota(jnp.int32, (owners, LANES), 0)
    b = lax.broadcasted_iota(jnp.int32, (owners, LANES), 1)
    at = (o >> stride) & (size - 1)
    place = at
    span = size
    for n, st, _ in near_axes:
        place = place + span * ((o >> st) & (n - 1))
        span *= n
    member = jnp.where((place == b) & (at != spot_ref[mine]), 1.0, 0.0)
    total = jnp.zeros((1, LANES), f32)
    for k in known:
        left = jnp.sum(k[:, fields - owners:fields], axis=0, keepdims=True)
        total = total + jnp.dot(left, member, preferred_element_type=f32)
    return jnp.max(jnp.where(total > room, 1.0, 0.0), axis=1, keepdims=True)


def first_body(near_axes, axis, room, owners, fields, width, cap, groups, spot_ref, prompt_ref, length_ref, level_ref, nth_ref, mark_ref, spill_ref, hold_ref, *rest):
    f32, i32 = jnp.float32, jnp.int32
    limit, half, _ = spill_ref.shape
    features = half * LANES
    send_refs, wide = rest[:-1], rest[-1]
    wide[...] = spill_ref[...].astype(f32)
    for c in range(half):
        hold_ref[:, c * LANES:(c + 1) * LANES] = wide[:, c, :].astype(jnp.bfloat16)
    hold_ref[:, features:features + LANES] = mark_ref[...]
    p, n = prompt_ref[...], length_ref[...]
    total = p.shape[1]
    owner = p >> log2(groups)
    place = nth_ref[...] * owners + owner
    column = jnp.broadcast_to(place.astype(f32), (total, total)).T.astype(i32)[:, :1]
    lane = lax.broadcasted_iota(i32, (total, width), 1)
    block = (fields - owners) // 3
    own = jnp.zeros((1, width), f32)
    for k, v in enumerate(((p & (groups - 1)) + 1, n, level_ref[...])):
        here = jnp.where(lane == column + k * block, 1.0, 0.0)
        own = own + jnp.dot(v.astype(f32), here, preferred_element_type=f32)
    here = jnp.where(lane == (column & (owners - 1)) + 3 * block, 1.0, 0.0)
    tokens = jnp.dot(n.astype(f32), here, preferred_element_type=f32)
    own = own + jnp.maximum(tokens - cap, 0.0)
    first = lax.broadcasted_iota(i32, (limit, width), 0) == 0
    known = jnp.where(first, own, 0.0)
    hold_ref[:, features + LANES:] = known.astype(jnp.bfloat16)
    left = jnp.sum(own[:, fields - owners:fields], axis=1, keepdims=True)
    bad = jnp.where(left > limit, 1.0, 0.0)
    bad = jnp.maximum(bad, crowding([known], owners, fields, near_axes, axis, room, spot_ref))
    moved = select([hold_ref], near_axes, axis, room, spot_ref, (features,))
    finish(moved, [known[:room]], bad, room, features, send_refs)


def finish(moved, known, bad, room, features, send_refs):
    rows = moved.shape[0]
    lane = lax.broadcasted_iota(jnp.int32, (rows, LANES), 1)
    info = jnp.where(lane == 4, bad, jnp.where(lane < 4, moved[:, features:], 0.0))
    for k, send_ref in enumerate(send_refs):
        part = slice(k * room, (k + 1) * room)
        send_ref[:, :features] = moved[part, :features].astype(jnp.bfloat16)
        send_ref[:, features:features + LANES] = info[part].astype(jnp.bfloat16)
        at = features + LANES
        for v in known:
            send_ref[:, at:at + v.shape[1]] = v.astype(jnp.bfloat16)
            at += v.shape[1]


def next_body(near_axes, axis, room, owners, fields, width, count, features, parts, recent, last, spot_ref, *refs):
    f32 = jnp.float32
    holds, own_ref, send_refs = refs[:parts], refs[parts], refs[parts + 1:]
    came = holds[parts - recent:]
    at = features + LANES
    blocks = (own_ref.shape[1] - at) // width
    bad = None
    known = []
    for i, ref in enumerate((own_ref, *came)):
        flag = jnp.max(ref[:, features:features + LANES].astype(f32)[:, 4:5], axis=0, keepdims=True)
        bad = flag if bad is None else jnp.maximum(bad, flag)
        for j in range(blocks):
            value = ref[:, at + j * width:at + (j + 1) * width].astype(f32)
            if count >= room:
                known.append(value)
                continue
            rows = ref.shape[0]
            to = lax.broadcasted_iota(jnp.int32, (room, rows), 0)
            source = lax.broadcasted_iota(jnp.int32, (room, rows), 1)
            shift = (i * count) % room
            put = jnp.where((to == source + shift) & (source < count), 1.0, 0.0)
            value = jnp.dot(put, value, preferred_element_type=f32)
            if (i * count) // room == len(known):
                known.append(value)
            else:
                known[-1] = known[-1] + value
    bad = jnp.maximum(bad, crowding(known, owners, fields, near_axes, axis, room, spot_ref))
    moved = select(holds, near_axes, axis, room, spot_ref, (features,))
    if not last:
        finish(moved, known, bad, room, features, send_refs)
        return
    token_ref, entry_ref, own_entry_ref = send_refs
    rows = len(known) * room
    for ref, who in ((own_entry_ref, spot_ref[0]), (entry_ref, spot_ref[0] ^ (1 << axis[1]))):
        lane = lax.broadcasted_iota(jnp.int32, (width, LANES), 0)
        column = lax.broadcasted_iota(jnp.int32, (width, LANES), 1)
        mine = jnp.where(((lane >> log2(owners)) == column) & ((lane & (owners - 1)) == who) & (lane < fields - owners), 1.0, 0.0)
        for j, v in enumerate(known):
            ref[j * room:(j + 1) * room, :] = jnp.dot(v, mine, preferred_element_type=f32).astype(jnp.bfloat16)
        lane = lax.broadcasted_iota(jnp.int32, (room, LANES), 1)
        info = jnp.where(lane == 4, bad, jnp.where(lane < 4, moved[:, features:], 0.0))
        ref[rows:rows + room, :] = info.astype(jnp.bfloat16)
    token_ref[...] = moved[:, :features].astype(jnp.bfloat16)


def plan_body(cap, full, slots, owners, features, main, room, batch, spot_ref, id_col_ref, id_row_ref, own_ref, got_ref, *refs):
    f32, i32 = jnp.float32, jnp.int32
    holds, (slot_ref, weight_ref, adv_ref, flag_ref) = refs[:-4], refs[-4:]
    rows = owners // 2
    total = slot_ref.shape[1]
    info = [ref[:, features:features + LANES].astype(f32) for ref in holds] + [got_ref[rows:rows + room, :].astype(f32)]
    bad = jnp.max(jnp.maximum(info[-1], own_ref[rows:rows + room, :].astype(f32)), axis=0, keepdims=True)
    bad = jnp.where(lax.broadcasted_iota(i32, (1, LANES), 1) == 4, bad, 0.0)
    flag_ref[0] = jnp.max(bad).astype(i32)
    there = jnp.concatenate(info, axis=0).T
    entry = jnp.concatenate([own_ref[:rows, :].astype(f32), got_ref[:rows, :].astype(f32)], axis=0)
    turned = entry.T
    ids, ids_row = id_col_ref[...], id_row_ref[...]
    label = [entry[:, k:k + 1] for k in range(slots)]
    size = [entry[:, slots + k:slots + k + 1] for k in range(slots)]
    level = [entry[:, 2 * slots + k:2 * slots + k + 1] for k in range(slots)]
    key = jnp.where((there[0:1] > 0) & (there[1:2] == spot_ref[0].astype(f32)), there[2:3] * 256.0 + there[3:4], -1.0)
    held_at = lax.broadcasted_iota(i32, (owners, key.shape[1]), 1).astype(f32)
    q = lax.broadcasted_iota(i32, (owners, total), 1).astype(f32)
    found = [jnp.zeros((owners, total), f32) for _ in range(5)]
    pos = jnp.zeros((owners, 1), f32)
    for k in range(slots):
        rank = jnp.zeros((owners, owners), f32)
        for j in range(slots):
            ahead = (ids_row < ids) if j >= k else (ids_row <= ids)
            rank = rank + jnp.where((label[k] == turned[j:j + 1, :]) & ahead, 1.0, 0.0)
        target = jnp.where(label[k] > 0, (label[k] - 1.0) * G + jnp.sum(rank, axis=1, keepdims=True), -1.0)
        places = []
        for t in range(2):
            p = pos if t == 0 else pos + jnp.where(size[k] > 1, 1.0, 0.0)
            place = ids * cap + p
            if 2 * k + t >= cap:
                held = jnp.sum(jnp.where(key == ids * 256.0 + p, held_at, 0.0), axis=1, keepdims=True)
                place = jnp.where(p < cap, place, main + held)
            places.append(place)
        hit = target == q
        for r, v in enumerate((*places, size[k], level[k], ids * full + pos)):
            found[r] = jnp.where(hit, v, found[r])
        pos = pos + size[k]
    one, two, n, lv, far = (jnp.sum(v, axis=0, keepdims=True) for v in found)
    a = lax.broadcasted_iota(i32, (total, total), 0)
    b = lax.broadcasted_iota(i32, (total, total), 1)
    spare = jnp.where(jnp.maximum(one, two) >= main, 1.0, 0.0)
    near = jnp.where(a >> log2(batch) == b >> log2(batch), 1.0, 0.0)
    slot_ref[0:1, :] = one.astype(i32)
    slot_ref[1:2, :] = two.astype(i32)
    slot_ref[2:3, :] = jnp.dot(spare, near, preferred_element_type=f32).astype(i32)
    slot_ref[3:4, :] = far.astype(i32)
    slot_ref[4:5, :] = (far + jnp.where(n > 1, 1.0, 0.0)).astype(i32)
    slot_ref[5:8, :] = jnp.zeros((3, total), i32)
    group = jnp.where(a >> log2(G) == b >> log2(G), 1.0, 0.0)
    mean = jnp.dot(lv, group, preferred_element_type=f32) * (1.0 / G)
    square = jnp.dot(lv * lv, group, preferred_element_type=f32) * (1.0 / G)
    spread = jnp.sqrt(square - mean * mean)
    advantage = (lv - mean) / jnp.maximum(spread, 1.0)
    adv_ref[...] = advantage
    weight_ref[0:1, :] = advantage / n
    weight_ref[1:2, :] = jnp.where(n > 1, advantage / n, 0.0)


def place_body(row, slot_ref, weight_ref, tokens_ref, *refs):
    f32 = jnp.float32
    holds, (out_ref, wide, out, extra, more, slot_s, weight_s, table_sems, out_sems) = refs[:-9], refs[-9:]
    copy_slot = pltpu.make_async_copy(slot_ref, slot_s, table_sems.at[0])
    copy_weight = pltpu.make_async_copy(weight_ref, weight_s, table_sems.at[1])
    copy_slot.start()
    copy_weight.start()
    pieces = out_sems.shape[0]
    main = tokens_ref.shape[0]
    batch, half = wide.shape[0], wide.shape[1] // 2
    base = 0
    for ref in holds:
        p = ref.shape[0]
        for c in range(half):
            extra[base:base + p, c, :] = ref[:, c * LANES:(c + 1) * LANES].astype(f32)
        base += p
    for h in range(base):
        more[h] = extra[h].astype(jnp.bfloat16)
    copy_slot.wait()
    copy_weight.wait()

    def work(j, mixed):
        for e in range(batch):
            i = j * batch + e
            for t in range(2):
                at = slot_s[row + t, i]
                if mixed:
                    x = tokens_ref[jnp.minimum(at, main - 1)]
                    x = jnp.where(at < main, x, more[jnp.maximum(at - main, 0)])
                else:
                    x = tokens_ref[at]
                wide[e, pl.ds(t, half, stride=2), :] = x.astype(f32) * weight_s[t, i]
        for e in range(batch):
            out[j * batch + e] = wide[e].astype(jnp.bfloat16)

    def chunk(k, _):
        if holds:
            @pl.when(slot_s[2, k * batch] == 0)
            def _():
                work(k, False)

            @pl.when(slot_s[2, k * batch] > 0)
            def _():
                work(k, True)
        else:
            work(k, False)
        part = pl.ds(k * batch, batch)
        pltpu.make_async_copy(out.at[part], out_ref.at[part], out_sems.at[k]).start()
        return 0

    lax.fori_loop(0, pieces, chunk, 0)
    for k in range(pieces):
        part = pl.ds(k * batch, batch)
        pltpu.make_async_copy(out.at[part], out_ref.at[part], out_sems.at[k]).wait()


SMEM = pl.BlockSpec(memory_space=pltpu.SMEM)
VMEM = pl.BlockSpec(memory_space=pltpu.VMEM)
HBM = pl.BlockSpec(memory_space=pltpu.HBM)
ROOM = pltpu.CompilerParams(vmem_limit_bytes=20 << 20)
COST = pl.CostEstimate(flops=1 << 20, bytes_accessed=1 << 20, transcendentals=0)


def pack(spot, rows, gain, prompt_of, lengths, owners, cap, groups, limit):
    total, width, _ = rows.shape
    half = width // 2
    few = max(limit, 16)
    return pl.pallas_call(
        functools.partial(pack_body, cap, groups, limit),
        out_shape=[
            jax.ShapeDtypeStruct((owners * cap, half, LANES), jnp.bfloat16),
            jax.ShapeDtypeStruct((few, half, LANES), jnp.bfloat16),
            jax.ShapeDtypeStruct((few, LANES), jnp.bfloat16),
            jax.ShapeDtypeStruct((1, total), jnp.int32),
        ],
        in_specs=[SMEM, VMEM, VMEM, VMEM, HBM],
        out_specs=[VMEM, VMEM, VMEM, VMEM],
        scratch_shapes=[
            pltpu.VMEM(rows.shape, jnp.bfloat16),
            pltpu.VMEM((BATCH, width, LANES), jnp.float32),
            pltpu.VMEM((2 * total, half, LANES), jnp.bfloat16),
            pltpu.VMEM((2, total), jnp.int32),
            pltpu.VMEM((few, LANES), jnp.int32),
            pltpu.SMEM((2, total), jnp.int32),
            pltpu.SMEM((few, LANES), jnp.int32),
            pltpu.SemaphoreType.DMA((4,)),
            pltpu.SemaphoreType.DMA((2,)),
        ],
        cost_estimate=COST, compiler_params=ROOM,
        name="pack",
    )(spot, prompt_of, lengths, gain, rows)


def log2(n):
    assert n & (n - 1) == 0
    return n.bit_length() - 1


def on_device(hidden, norm_gain, prompt_of, lengths, reward_level):
    f32, i32, bf16 = jnp.float32, jnp.int32, jnp.bfloat16
    count_here, window, features = hidden.shape
    sizes = {a: lax.axis_size(a) for a in AXES}
    owners = sizes["gx"] * sizes["gy"] * sizes["gz"]
    slots = max(2, count_here // owners + 1)
    mean = window * count_here // owners
    full = window * slots
    cap = min(full, max(window, mean - mean // 8))
    limit, room = 16, 8
    groups = count_here // G
    half = features // LANES
    stride = {"gx": sizes["gy"] * sizes["gz"], "gy": sizes["gz"], "gz": 1}
    coord = {a: lax.axis_index(a) for a in AXES}
    me = sum(coord[a] * stride[a] for a in AXES)
    stages = [("gz", 0, sizes["gz"]), ("gx", 0, sizes["gx"])]
    stages += [("gy", bit, 2) for bit in range(log2(sizes["gy"]))]
    spot = jnp.stack([me] + [(coord[a] >> bit) & (n - 1) for a, bit, n in stages]).astype(i32)
    fields = 3 * slots * owners + owners
    width = -(-fields // LANES) * LANES

    rows = hidden.reshape(count_here, window, half, LANES).transpose(0, 2, 1, 3)
    rows = rows.reshape(count_here, window * half, LANES)
    gain = norm_gain.reshape(half, LANES)
    prompts, sizes_of, levels = prompt_of[None], lengths[None], reward_level[None]
    sent, spill, marks, nth = pack(spot, rows, gain, prompts, sizes_of, owners, cap, groups, limit)
    came = lax.all_to_all(sent, AXES, split_axis=0, concat_axis=0, tiled=True)

    lanes = features + LANES
    shape = functools.partial(jax.ShapeDtypeStruct, dtype=bf16)
    holds, got, own, near, count, before = [], [], None, [], 1, 0
    steps = {a: np.zeros((1,), np.int32) for a in AXES}
    for n, (a, bit, size) in enumerate(stages):
        axis = (size, log2(stride[a]) + bit, n + 1)
        if n == 0:
            hold, *sends = pl.pallas_call(
                functools.partial(first_body, tuple(near), axis, room, owners, fields, width, cap, groups),
                out_shape=[shape((limit, lanes + width))] + [shape((room, lanes + width))] * (size - 1),
                in_specs=[SMEM] + [VMEM] * 6, out_specs=[VMEM] * size,
                scratch_shapes=[pltpu.VMEM((limit, half, LANES), f32)],
                cost_estimate=COST, compiler_params=ROOM, name="stage",
            )(spot, prompts, sizes_of, levels, nth, marks, spill)
            holds = [hold]
        else:
            blocks = -(-count // room)
            last = n + 1 == len(stages)
            outs = [shape((room, lanes + blocks * width))] * (size - 1)
            if last:
                outs = [shape((room, features)), shape((count + room, LANES)), shape((count + room, LANES))]
            sends = pl.pallas_call(
                functools.partial(next_body, tuple(near), axis, room, owners, fields, width, before, features, len(holds), len(got), last),
                out_shape=outs,
                in_specs=[SMEM] + [VMEM] * (len(holds) + 1), out_specs=[VMEM] * len(outs),
                cost_estimate=COST, compiler_params=ROOM, name="stage",
            )(spot, *holds, own)
        pairs = [[(i, i ^ (k << bit)) for i in range(sizes[a])] for k in range(size)]
        if n + 1 < len(stages):
            got = [lax.ppermute(sends[k - 1], a, pairs[k]) for k in range(1, size)]
            own = sends[0]
            holds = holds + got
        else:
            own = sends[2]
            entries = lax.ppermute(sends[1], a, pairs[1])
            landed = lax.ppermute(sends[0], a, pairs[1])
        near.append(axis)
        before = count
        count *= size
        steps = {x: np.concatenate([v + ((k << bit) if x == a else 0) for k in range(size)]).astype(np.int32) for x, v in steps.items()}

    ids = sum((coord[a] ^ steps[a]) * stride[a] for a in AXES).astype(f32)
    batch = min(16, count_here)
    vmem_i32 = functools.partial(jax.ShapeDtypeStruct, dtype=i32)
    slot_of, weight, advantages, bad = pl.pallas_call(
        functools.partial(plan_body, cap, full, slots, owners, features, owners * cap, room, batch),
        out_shape=[vmem_i32((8, count_here)), jax.ShapeDtypeStruct((window, count_here), f32), jax.ShapeDtypeStruct((1, count_here), f32), vmem_i32((1,))],
        in_specs=[SMEM] + [VMEM] * (4 + len(holds)), out_specs=[VMEM, VMEM, VMEM, SMEM],
        cost_estimate=COST, compiler_params=ROOM, name="plan",
    )(spot, ids[:, None], ids[None], own, entries, *holds)

    def place(tokens, row, extras):
        spare = max(sum(h.shape[0] for h in extras), 8)
        return pl.pallas_call(
            functools.partial(place_body, row),
            out_shape=jax.ShapeDtypeStruct((count_here, window * half, LANES), bf16),
            in_specs=[VMEM] * (3 + len(extras)), out_specs=HBM,
            scratch_shapes=[
                pltpu.VMEM((batch, window * half, LANES), f32),
                pltpu.VMEM((count_here, window * half, LANES), bf16),
                pltpu.VMEM((spare, half, LANES), f32),
                pltpu.VMEM((spare, half, LANES), bf16),
                pltpu.SMEM((8, count_here), i32),
                pltpu.SMEM((window, count_here), f32),
                pltpu.SemaphoreType.DMA((2,)),
                pltpu.SemaphoreType.DMA((count_here // batch,)),
            ],
            cost_estimate=COST, compiler_params=ROOM, name="place",
        )(slot_of, weight, tokens, *extras)

    def whole(out):
        out = out.reshape(count_here, half, window, LANES).transpose(0, 2, 1, 3)
        return out.reshape(count_here, window, features)

    out = place(came, 0, [*holds, landed])

    def crowded(state):
        again = pack(spot, rows, gain, prompts, sizes_of, owners, full, groups, 0)
        all_came = lax.all_to_all(again[0], AXES, split_axis=0, concat_axis=0, tiled=True)
        return jnp.zeros((1,), i32), whole(place(all_came, 3, []))

    _, out = lax.while_loop(lambda state: state[0][0] > 0, crowded, (bad, whole(out)))
    return out, advantages.reshape(count_here)


def solution(mesh):
    many = P(AXES)
    return jax.shard_map(
        on_device, mesh=mesh,
        in_specs=(P(AXES, None, None), P(), many, many, many),
        out_specs=(P(AXES, None, None), many), check_vma=False,
    )
```

```python
import functools
import jax
import numpy as np
import jax.numpy as jnp
from jax import lax
from jax.experimental import pallas as pl
from jax.experimental.pallas import tpu as pltpu
from jax.sharding import PartitionSpec as P

G = 16
AXES = ("gx", "gy", "gz")
LANES = 128
BATCH = 32
norm_eps = 1e-05


def pack_body(cap, groups, limit, spot_ref, prompt_ref, length_ref, gain_ref, rows_ref,
              out_ref, spill_ref, mark_ref, nth_ref,
              rows, wide, tokens, way_v, list_v, way, spilled, in_sems, way_sems):
    f32, i32 = jnp.float32, jnp.int32
    total, pieces = rows.shape[0], in_sems.shape[0]
    piece = total // pieces
    batch = wide.shape[0]
    half = wide.shape[1] // 2
    features = half * LANES
    for k in range(pieces):
        part = pl.ds(k * piece, piece)
        pltpu.make_async_copy(rows_ref.at[part], rows.at[part], in_sems.at[k]).start()

    p, n = prompt_ref[...], length_ref[...]
    column = jnp.broadcast_to((p * 4 + n).astype(f32), (total, total)).T.astype(i32)
    before = lax.broadcasted_iota(i32, (total, total), 0) < lax.broadcasted_iota(i32, (total, total), 1)
    owner = p >> log2(groups)
    same = ((column >> (2 + log2(groups))) == owner) & before
    at = jnp.sum(jnp.where(same, column & 3, 0), axis=0, keepdims=True)
    nth_ref[...] = jnp.sum(jnp.where(same, 1, 0), axis=0, keepdims=True)
    lane = lax.broadcasted_iota(i32, (1, total), 1)
    home = jnp.sum(jnp.where(lane == 0, owner, 0), axis=1, keepdims=True) * cap
    d0 = jnp.where(at < cap, owner * cap + at, home)
    way_v[0:1, :] = d0
    way_v[1:2, :] = jnp.where((n > 1) & (at + 1 < cap), d0 + 1, d0)
    pltpu.make_async_copy(way_v, way, way_sems.at[0]).start()
    if limit:
        over = jnp.where(at >= cap, 1, 0)
        more = jnp.where((n > 1) & (at + 1 >= cap), 1, 0)
        start = jnp.dot((over + more).astype(f32), jnp.where(before, 1.0, 0.0), preferred_element_type=f32).astype(i32)
        e = lax.broadcasted_iota(i32, (limit, total), 0)
        hit0 = (over > 0) & (start == e)
        hit1 = (more > 0) & (start + over == e)
        token = jnp.sum(jnp.where(hit0, 2 * lane + 1, jnp.where(hit1, 2 * lane + 2, 0)), axis=1, keepdims=True)
        dest = jnp.sum(jnp.where(hit0 | hit1, owner, 0), axis=1, keepdims=True)
        spot = jnp.sum(jnp.where(hit0, at, jnp.where(hit1, at + 1, 0)), axis=1, keepdims=True)
        lanes = lax.broadcasted_iota(i32, (limit, LANES), 1)
        mark = jnp.where(lanes == 0, 1, jnp.where(lanes == 1, dest, jnp.where(lanes == 2, spot_ref[0], jnp.where(lanes == 3, spot, 0))))
        mark_ref[...] = jnp.where(token > 0, mark, 0).astype(f32).astype(jnp.bfloat16)
        list_v[...] = jnp.broadcast_to(jnp.maximum(token - 1, 0), list_v.shape)
        pltpu.make_async_copy(list_v, spilled, way_sems.at[1]).start()
    else:
        mark_ref[...] = jnp.zeros(mark_ref.shape, mark_ref.dtype)
    gain = gain_ref[...]
    pltpu.make_async_copy(way_v, way, way_sems.at[0]).wait()

    def work(j, _):
        for b in range(batch):
            wide[b] = rows[j * batch + b].astype(f32)
        for b in range(batch):
            i = j * batch + b
            for t in (1, 0):
                x = wide[b, pl.ds(t, half, stride=2), :]
                s = jnp.sum((x * x).reshape(half // 8, 8, LANES), axis=0)
                s = jnp.sum(jnp.sum(s, axis=1, keepdims=True), axis=0, keepdims=True)
                r = lax.rsqrt(s * (1.0 / features) + norm_eps)
                x = (x * r * gain).astype(jnp.bfloat16)
                out_ref[way[t, i]] = x
                tokens[2 * i + t] = x
        return 0

    per = piece // batch

    def chunk(k, _):
        part = pl.ds(k * piece, piece)
        pltpu.make_async_copy(rows_ref.at[part], rows.at[part], in_sems.at[k]).wait()
        return lax.fori_loop(k * per, (k + 1) * per, work, 0)

    lax.fori_loop(0, pieces, chunk, 0)
    out_ref[way[0, 0]] = tokens[0]
    if limit:
        pltpu.make_async_copy(list_v, spilled, way_sems.at[1]).wait()
        for e in range(limit):
            spill_ref[e] = tokens[spilled[e, 0]]
    else:
        spill_ref[...] = jnp.zeros(spill_ref.shape, spill_ref.dtype)


def select(parts, near_axes, axis, room, spot_ref, shape):
    f32 = jnp.float32
    size, stride, mine = axis
    moved, offset = None, jnp.zeros((1, LANES), f32)
    for ref in parts:
        p = ref.shape[0]
        info = ref[:, shape[0]:shape[0] + LANES].astype(f32)
        dest = info[:, 1:2].astype(jnp.int32)
        lane = lax.broadcasted_iota(jnp.int32, (p, LANES), 1)
        go = (lane < (size - 1) * room) & (info[:, 0:1] > 0)
        for n, st, at in near_axes:
            go = go & (((dest >> st) & (n - 1)) == spot_ref[at])
        turn = lane & (room - 1)
        to = spot_ref[mine] ^ ((lane >> (room.bit_length() - 1)) + 1)
        go = jnp.where(go & (((dest >> stride) & (size - 1)) == to), 1.0, 0.0)
        row = lax.broadcasted_iota(jnp.int32, (p, p), 0)
        col = lax.broadcasted_iota(jnp.int32, (p, p), 1)
        nth = jnp.dot(jnp.where(col < row, 1.0, 0.0), go, preferred_element_type=f32) + offset
        offset = offset + jnp.sum(go, axis=0, keepdims=True)
        pick = jnp.where(nth == turn.astype(f32), go, 0.0)[:, :(size - 1) * room]
        data = ref[:, :shape[0] + LANES].astype(f32)
        part = lax.dot_general(pick, data, (((0,), (0,)), ((), ())), preferred_element_type=f32)
        moved = part if moved is None else moved + part
    return moved


def crowding(known, owners, fields, near_axes, axis, room, spot_ref):
    f32 = jnp.float32
    size, stride, mine = axis
    o = lax.broadcasted_iota(jnp.int32, (owners, LANES), 0)
    b = lax.broadcasted_iota(jnp.int32, (owners, LANES), 1)
    at = (o >> stride) & (size - 1)
    place = at
    span = size
    for n, st, _ in near_axes:
        place = place + span * ((o >> st) & (n - 1))
        span *= n
    member = jnp.where((place == b) & (at != spot_ref[mine]), 1.0, 0.0)
    total = jnp.zeros((1, LANES), f32)
    for k in known:
        left = jnp.sum(k[:, fields - owners:fields], axis=0, keepdims=True)
        total = total + jnp.dot(left, member, preferred_element_type=f32)
    return jnp.max(jnp.where(total > room, 1.0, 0.0), axis=1, keepdims=True)


def first_body(near_axes, axis, room, owners, fields, width, cap, groups, spot_ref, prompt_ref, length_ref, level_ref, nth_ref, mark_ref, spill_ref, hold_ref, *rest):
    f32, i32 = jnp.float32, jnp.int32
    limit, half, _ = spill_ref.shape
    features = half * LANES
    send_refs, wide = rest[:-1], rest[-1]
    wide[...] = spill_ref[...].astype(f32)
    for c in range(half):
        hold_ref[:, c * LANES:(c + 1) * LANES] = wide[:, c, :].astype(jnp.bfloat16)
    hold_ref[:, features:features + LANES] = mark_ref[...]
    p, n = prompt_ref[...], length_ref[...]
    total = p.shape[1]
    owner = p >> log2(groups)
    place = nth_ref[...] * owners + owner
    column = jnp.broadcast_to(place.astype(f32), (total, total)).T.astype(i32)[:, :1]
    lane = lax.broadcasted_iota(i32, (total, width), 1)
    block = (fields - owners) // 3
    own = jnp.zeros((1, width), f32)
    for k, v in enumerate(((p & (groups - 1)) + 1, n, level_ref[...])):
        here = jnp.where(lane == column + k * block, 1.0, 0.0)
        own = own + jnp.dot(v.astype(f32), here, preferred_element_type=f32)
    here = jnp.where(lane == (column & (owners - 1)) + 3 * block, 1.0, 0.0)
    tokens = jnp.dot(n.astype(f32), here, preferred_element_type=f32)
    own = own + jnp.maximum(tokens - cap, 0.0)
    first = lax.broadcasted_iota(i32, (limit, width), 0) == 0
    known = jnp.where(first, own, 0.0)
    hold_ref[:, features + LANES:] = known.astype(jnp.bfloat16)
    left = jnp.sum(own[:, fields - owners:fields], axis=1, keepdims=True)
    bad = jnp.where(left > limit, 1.0, 0.0)
    bad = jnp.maximum(bad, crowding([known], owners, fields, near_axes, axis, room, spot_ref))
    moved = select([hold_ref], near_axes, axis, room, spot_ref, (features,))
    finish(moved, [known[:room]], bad, room, features, send_refs)


def finish(moved, known, bad, room, features, send_refs):
    rows = moved.shape[0]
    lane = lax.broadcasted_iota(jnp.int32, (rows, LANES), 1)
    info = jnp.where(lane == 4, bad, jnp.where(lane < 4, moved[:, features:], 0.0))
    for k, send_ref in enumerate(send_refs):
        part = slice(k * room, (k + 1) * room)
        send_ref[:, :features] = moved[part, :features].astype(jnp.bfloat16)
        send_ref[:, features:features + LANES] = info[part].astype(jnp.bfloat16)
        at = features + LANES
        for v in known:
            send_ref[:, at:at + v.shape[1]] = v.astype(jnp.bfloat16)
            at += v.shape[1]


def next_body(near_axes, axis, room, owners, fields, width, count, features, parts, recent, last, spot_ref, *refs):
    f32 = jnp.float32
    holds, own_ref, send_refs = refs[:parts], refs[parts], refs[parts + 1:]
    came = holds[parts - recent:]
    at = features + LANES
    blocks = (own_ref.shape[1] - at) // width
    bad = None
    known = []
    for i, ref in enumerate((own_ref, *came)):
        flag = jnp.max(ref[:, features:features + LANES].astype(f32)[:, 4:5], axis=0, keepdims=True)
        bad = flag if bad is None else jnp.maximum(bad, flag)
        for j in range(blocks):
            value = ref[:, at + j * width:at + (j + 1) * width].astype(f32)
            if count >= room:
                known.append(value)
                continue
            rows = ref.shape[0]
            to = lax.broadcasted_iota(jnp.int32, (room, rows), 0)
            source = lax.broadcasted_iota(jnp.int32, (room, rows), 1)
            shift = (i * count) % room
            put = jnp.where((to == source + shift) & (source < count), 1.0, 0.0)
            value = jnp.dot(put, value, preferred_element_type=f32)
            if (i * count) // room == len(known):
                known.append(value)
            else:
                known[-1] = known[-1] + value
    seats = 2 * send_refs[0].shape[0] if last else room
    bad = jnp.maximum(bad, crowding(known, owners, fields, near_axes, axis, seats, spot_ref))
    moved = select(holds, near_axes, axis, room, spot_ref, (features,))
    if not last:
        finish(moved, known, bad, room, features, send_refs)
        return
    token_ref, entry_ref, own_entry_ref = send_refs
    rows = len(known) * room
    for ref, who in ((own_entry_ref, spot_ref[0]), (entry_ref, spot_ref[0] ^ (1 << axis[1]))):
        lane = lax.broadcasted_iota(jnp.int32, (width, LANES), 0)
        column = lax.broadcasted_iota(jnp.int32, (width, LANES), 1)
        mine = jnp.where(((lane >> log2(owners)) == column) & ((lane & (owners - 1)) == who) & (lane < fields - owners), 1.0, 0.0)
        for j, v in enumerate(known):
            ref[j * room:(j + 1) * room, :] = jnp.dot(v, mine, preferred_element_type=f32).astype(jnp.bfloat16)
        lane = lax.broadcasted_iota(jnp.int32, (room, LANES), 1)
        info = jnp.where(lane == 4, bad, jnp.where(lane < 4, moved[:, features:], 0.0))
        ref[rows:rows + room, :] = info.astype(jnp.bfloat16)
    for i in range(token_ref.shape[0]):
        token_ref[i] = moved[2 * i:2 * i + 2, :features].astype(jnp.bfloat16)


def plan_body(cap, full, slots, owners, features, main, room, batch, spot_ref, id_col_ref, id_row_ref, own_ref, got_ref, *refs):
    f32, i32 = jnp.float32, jnp.int32
    holds, (slot_ref, weight_ref, adv_ref, flag_ref) = refs[:-4], refs[-4:]
    rows = owners // 2
    total = slot_ref.shape[1]
    info = [ref[:, features:features + LANES].astype(f32) for ref in holds] + [got_ref[rows:rows + room, :].astype(f32)]
    bad = jnp.max(jnp.maximum(info[-1], own_ref[rows:rows + room, :].astype(f32)), axis=0, keepdims=True)
    bad = jnp.where(lax.broadcasted_iota(i32, (1, LANES), 1) == 4, bad, 0.0)
    flag_ref[0] = jnp.max(bad).astype(i32)
    there = jnp.concatenate(info, axis=0).T
    entry = jnp.concatenate([own_ref[:rows, :].astype(f32), got_ref[:rows, :].astype(f32)], axis=0)
    turned = entry.T
    ids, ids_row = id_col_ref[...], id_row_ref[...]
    label = [entry[:, k:k + 1] for k in range(slots)]
    size = [entry[:, slots + k:slots + k + 1] for k in range(slots)]
    level = [entry[:, 2 * slots + k:2 * slots + k + 1] for k in range(slots)]
    key = jnp.where((there[0:1] > 0) & (there[1:2] == spot_ref[0].astype(f32)), there[2:3] * 256.0 + there[3:4], -1.0)
    held_at = lax.broadcasted_iota(i32, (owners, key.shape[1]), 1).astype(f32)
    q = lax.broadcasted_iota(i32, (owners, total), 1).astype(f32)
    found = [jnp.zeros((owners, total), f32) for _ in range(5)]
    pos = jnp.zeros((owners, 1), f32)
    for k in range(slots):
        rank = jnp.zeros((owners, owners), f32)
        for j in range(slots):
            ahead = (ids_row < ids) if j >= k else (ids_row <= ids)
            rank = rank + jnp.where((label[k] == turned[j:j + 1, :]) & ahead, 1.0, 0.0)
        target = jnp.where(label[k] > 0, (label[k] - 1.0) * G + jnp.sum(rank, axis=1, keepdims=True), -1.0)
        places = []
        for t in range(2):
            p = pos if t == 0 else pos + jnp.where(size[k] > 1, 1.0, 0.0)
            place = ids * cap + p
            if 2 * k + t >= cap:
                held = jnp.sum(jnp.where(key == ids * 256.0 + p, held_at, 0.0), axis=1, keepdims=True)
                place = jnp.where(p < cap, place, main + held)
            places.append(place)
        hit = target == q
        for r, v in enumerate((*places, size[k], level[k], ids * full + pos)):
            found[r] = jnp.where(hit, v, found[r])
        pos = pos + size[k]
    one, two, n, lv, far = (jnp.sum(v, axis=0, keepdims=True) for v in found)
    a = lax.broadcasted_iota(i32, (total, total), 0)
    b = lax.broadcasted_iota(i32, (total, total), 1)
    spare = jnp.where(jnp.maximum(one, two) >= main, 1.0, 0.0)
    near = jnp.where(a >> log2(batch) == b >> log2(batch), 1.0, 0.0)
    slot_ref[0:1, :] = one.astype(i32)
    slot_ref[1:2, :] = two.astype(i32)
    slot_ref[2:3, :] = jnp.dot(spare, near, preferred_element_type=f32).astype(i32)
    slot_ref[3:4, :] = far.astype(i32)
    slot_ref[4:5, :] = (far + jnp.where(n > 1, 1.0, 0.0)).astype(i32)
    slot_ref[5:8, :] = jnp.zeros((3, total), i32)
    group = jnp.where(a >> log2(G) == b >> log2(G), 1.0, 0.0)
    mean = jnp.dot(lv, group, preferred_element_type=f32) * (1.0 / G)
    square = jnp.dot(lv * lv, group, preferred_element_type=f32) * (1.0 / G)
    spread = jnp.sqrt(square - mean * mean)
    advantage = (lv - mean) / jnp.maximum(spread, 1.0)
    adv_ref[...] = advantage
    weight_ref[0:1, :] = advantage / n
    weight_ref[1:2, :] = jnp.where(n > 1, advantage / n, 0.0)


def place_body(row, slot_ref, weight_ref, tokens_ref, *refs):
    f32 = jnp.float32
    holds, (out_ref, wide, out, extra, more, slot_s, weight_s, table_sems, out_sems) = refs[:-9], refs[-9:]
    copy_slot = pltpu.make_async_copy(slot_ref, slot_s, table_sems.at[0])
    copy_weight = pltpu.make_async_copy(weight_ref, weight_s, table_sems.at[1])
    copy_slot.start()
    copy_weight.start()
    pieces = out_sems.shape[0]
    main = tokens_ref.shape[0]
    batch, half = wide.shape[0], wide.shape[1] // 2
    base = 0
    for ref in holds:
        for piece in ([ref] if len(ref.shape) == 2 else [ref.at[i] for i in range(ref.shape[0])]):
            p = piece.shape[0]
            for c in range(half):
                extra[base:base + p, c, :] = piece[:, c * LANES:(c + 1) * LANES].astype(f32)
            base += p
    for h in range(base):
        more[h] = extra[h].astype(jnp.bfloat16)
    copy_slot.wait()
    copy_weight.wait()

    def work(j, mixed):
        for e in range(batch):
            i = j * batch + e
            for t in range(2):
                at = slot_s[row + t, i]
                if mixed:
                    x = tokens_ref[jnp.minimum(at, main - 1)]
                    x = jnp.where(at < main, x, more[jnp.maximum(at - main, 0)])
                else:
                    x = tokens_ref[at]
                wide[e, pl.ds(t, half, stride=2), :] = x.astype(f32) * weight_s[t, i]
        for e in range(batch):
            out[j * batch + e] = wide[e].astype(jnp.bfloat16)

    def chunk(k, _):
        if holds:
            @pl.when(slot_s[2, k * batch] == 0)
            def _():
                work(k, False)

            @pl.when(slot_s[2, k * batch] > 0)
            def _():
                work(k, True)
        else:
            work(k, False)
        part = pl.ds(k * batch, batch)
        pltpu.make_async_copy(out.at[part], out_ref.at[part], out_sems.at[k]).start()
        return 0

    lax.fori_loop(0, pieces, chunk, 0)
    for k in range(pieces):
        part = pl.ds(k * batch, batch)
        pltpu.make_async_copy(out.at[part], out_ref.at[part], out_sems.at[k]).wait()


SMEM = pl.BlockSpec(memory_space=pltpu.SMEM)
VMEM = pl.BlockSpec(memory_space=pltpu.VMEM)
HBM = pl.BlockSpec(memory_space=pltpu.HBM)
ROOM = pltpu.CompilerParams(vmem_limit_bytes=20 << 20)
COST = pl.CostEstimate(flops=1 << 20, bytes_accessed=1 << 20, transcendentals=0)


def pack(spot, rows, gain, prompt_of, lengths, owners, cap, groups, limit):
    total, width, _ = rows.shape
    half = width // 2
    few = max(limit, 16)
    return pl.pallas_call(
        functools.partial(pack_body, cap, groups, limit),
        out_shape=[
            jax.ShapeDtypeStruct((owners * cap, half, LANES), jnp.bfloat16),
            jax.ShapeDtypeStruct((few, half, LANES), jnp.bfloat16),
            jax.ShapeDtypeStruct((few, LANES), jnp.bfloat16),
            jax.ShapeDtypeStruct((1, total), jnp.int32),
        ],
        in_specs=[SMEM, VMEM, VMEM, VMEM, HBM],
        out_specs=[VMEM, VMEM, VMEM, VMEM],
        scratch_shapes=[
            pltpu.VMEM(rows.shape, jnp.bfloat16),
            pltpu.VMEM((BATCH, width, LANES), jnp.float32),
            pltpu.VMEM((2 * total, half, LANES), jnp.bfloat16),
            pltpu.VMEM((2, total), jnp.int32),
            pltpu.VMEM((few, LANES), jnp.int32),
            pltpu.SMEM((2, total), jnp.int32),
            pltpu.SMEM((few, LANES), jnp.int32),
            pltpu.SemaphoreType.DMA((4,)),
            pltpu.SemaphoreType.DMA((2,)),
        ],
        cost_estimate=COST, compiler_params=ROOM,
        name="pack",
    )(spot, prompt_of, lengths, gain, rows)


def log2(n):
    assert n & (n - 1) == 0
    return n.bit_length() - 1


def on_device(hidden, norm_gain, prompt_of, lengths, reward_level):
    f32, i32, bf16 = jnp.float32, jnp.int32, jnp.bfloat16
    count_here, window, features = hidden.shape
    sizes = {a: lax.axis_size(a) for a in AXES}
    owners = sizes["gx"] * sizes["gy"] * sizes["gz"]
    slots = max(2, count_here // owners + 1)
    mean = window * count_here // owners
    full = window * slots
    cap = min(full, max(window, mean - mean // 8))
    limit, room = 16, 8
    groups = count_here // G
    half = features // LANES
    stride = {"gx": sizes["gy"] * sizes["gz"], "gy": sizes["gz"], "gz": 1}
    coord = {a: lax.axis_index(a) for a in AXES}
    me = sum(coord[a] * stride[a] for a in AXES)
    stages = [("gz", 0, sizes["gz"]), ("gx", 0, sizes["gx"])]
    stages += [("gy", bit, 2) for bit in range(log2(sizes["gy"]))]
    spot = jnp.stack([me] + [(coord[a] >> bit) & (n - 1) for a, bit, n in stages]).astype(i32)
    fields = 3 * slots * owners + owners
    width = -(-fields // LANES) * LANES

    rows = hidden.reshape(count_here, window, half, LANES).transpose(0, 2, 1, 3)
    rows = rows.reshape(count_here, window * half, LANES)
    gain = norm_gain.reshape(half, LANES)
    prompts, sizes_of, levels = prompt_of[None], lengths[None], reward_level[None]
    sent, spill, marks, nth = pack(spot, rows, gain, prompts, sizes_of, owners, cap, groups, limit)
    came = lax.all_to_all(sent, AXES, split_axis=0, concat_axis=0, tiled=True)

    lanes = features + LANES
    shape = functools.partial(jax.ShapeDtypeStruct, dtype=bf16)
    holds, got, own, near, count, before = [], [], None, [], 1, 0
    steps = {a: np.zeros((1,), np.int32) for a in AXES}
    for n, (a, bit, size) in enumerate(stages):
        axis = (size, log2(stride[a]) + bit, n + 1)
        if n == 0:
            hold, *sends = pl.pallas_call(
                functools.partial(first_body, tuple(near), axis, room, owners, fields, width, cap, groups),
                out_shape=[shape((limit, lanes + width))] + [shape((room, lanes + width))] * (size - 1),
                in_specs=[SMEM] + [VMEM] * 6, out_specs=[VMEM] * size,
                scratch_shapes=[pltpu.VMEM((limit, half, LANES), f32)],
                cost_estimate=COST, compiler_params=ROOM, name="stage",
            )(spot, prompts, sizes_of, levels, nth, marks, spill)
            holds = [hold]
        else:
            blocks = -(-count // room)
            last = n + 1 == len(stages)
            outs = [shape((room, lanes + blocks * width))] * (size - 1)
            if last:
                outs = [shape((room // 2 - room // 8, 2, features)), shape((count + room, LANES)), shape((count + room, LANES))]
            sends = pl.pallas_call(
                functools.partial(next_body, tuple(near), axis, room, owners, fields, width, before, features, len(holds), len(got), last),
                out_shape=outs,
                in_specs=[SMEM] + [VMEM] * (len(holds) + 1), out_specs=[VMEM] * len(outs),
                cost_estimate=COST, compiler_params=ROOM, name="stage",
            )(spot, *holds, own)
        pairs = [[(i, i ^ (k << bit)) for i in range(sizes[a])] for k in range(size)]
        if n + 1 < len(stages):
            got = [lax.ppermute(sends[k - 1], a, pairs[k]) for k in range(1, size)]
            own = sends[0]
            holds = holds + got
        else:
            own = sends[2]
            entries = lax.ppermute(sends[1], a, pairs[1])
            landed = lax.ppermute(sends[0], a, pairs[1])
        near.append(axis)
        before = count
        count *= size
        steps = {x: np.concatenate([v + ((k << bit) if x == a else 0) for k in range(size)]).astype(np.int32) for x, v in steps.items()}

    ids = sum((coord[a] ^ steps[a]) * stride[a] for a in AXES).astype(f32)
    batch = min(16, count_here)
    vmem_i32 = functools.partial(jax.ShapeDtypeStruct, dtype=i32)
    slot_of, weight, advantages, bad = pl.pallas_call(
        functools.partial(plan_body, cap, full, slots, owners, features, owners * cap, room, batch),
        out_shape=[vmem_i32((8, count_here)), jax.ShapeDtypeStruct((window, count_here), f32), jax.ShapeDtypeStruct((1, count_here), f32), vmem_i32((1,))],
        in_specs=[SMEM] + [VMEM] * (4 + len(holds)), out_specs=[VMEM, VMEM, VMEM, SMEM],
        cost_estimate=COST, compiler_params=ROOM, name="plan",
    )(spot, ids[:, None], ids[None], own, entries, *holds)

    def place(tokens, row, extras):
        spare = max(sum(h.size // features if h.ndim == 3 else h.shape[0] for h in extras), 8)
        return pl.pallas_call(
            functools.partial(place_body, row),
            out_shape=jax.ShapeDtypeStruct((count_here, window * half, LANES), bf16),
            in_specs=[VMEM] * (3 + len(extras)), out_specs=HBM,
            scratch_shapes=[
                pltpu.VMEM((batch, window * half, LANES), f32),
                pltpu.VMEM((count_here, window * half, LANES), bf16),
                pltpu.VMEM((spare, half, LANES), f32),
                pltpu.VMEM((spare, half, LANES), bf16),
                pltpu.SMEM((8, count_here), i32),
                pltpu.SMEM((window, count_here), f32),
                pltpu.SemaphoreType.DMA((2,)),
                pltpu.SemaphoreType.DMA((count_here // batch,)),
            ],
            cost_estimate=COST, compiler_params=ROOM, name="place",
        )(slot_of, weight, tokens, *extras)

    def whole(out):
        out = out.reshape(count_here, half, window, LANES).transpose(0, 2, 1, 3)
        return out.reshape(count_here, window, features)

    out = place(came, 0, [*holds, landed])

    def crowded(state):
        again = pack(spot, rows, gain, prompts, sizes_of, owners, full, groups, 0)
        all_came = lax.all_to_all(again[0], AXES, split_axis=0, concat_axis=0, tiled=True)
        return jnp.zeros((1,), i32), whole(place(all_came, 3, []))

    _, out = lax.while_loop(lambda state: state[0][0] > 0, crowded, (bad, whole(out)))
    return out, advantages.reshape(count_here)


def solution(mesh):
    many = P(AXES)
    return jax.shard_map(
        on_device, mesh=mesh,
        in_specs=(P(AXES, None, None), P(), many, many, many),
        out_specs=(P(AXES, None, None), many), check_vma=False,
    )
```
